32 devices in a mesh: batch: 1 (over z), col: 4 (over y), row: 8 (over x, core).
Axes of the slice: x: 4, y: 4, z: 1, core: 2. Of those that a mesh axis runs over, the one named last changes fastest.
The devices are a block of a 4x4x8 slice.
Arguments:
- mat_blocks: float32 [32768, 128, 32], P(('batch', 'row'), 'col')
Outputs:
- output 1: float32 [32768, 128, 32], P(('batch', 'row'), 'col')
- output 2: float32 [128], P('batch')
- output 3: float32 [4, 32, 32], P('batch')
All inputs are finite; a program needn't handle non-finite values.
Results may differ from the reference program's by a relative error of at most 0.001.
Values sent between devices are 32-bit elements.
A program may use at most 768 MiB of HBM per device.

```python
import math
import jax
import jax.numpy as jnp
from jax import lax

MATRIX_ROWS = 32768
MATRIX_COLS = 4096
BLOCK_COLS = 32
PANELS = 4
COL_PROCS = 4
PANEL_COLS = PANELS * BLOCK_COLS
TOTAL_BLOCKS = MATRIX_COLS // BLOCK_COLS
LOCAL_BLOCKS = TOTAL_BLOCKS // COL_PROCS
HIGHEST = lax.Precision.HIGHEST


def mat_dot(left_mat, right_mat):
    return jnp.dot(left_mat, right_mat, precision=HIGHEST, preferred_element_type=jnp.float32)


def to_stored(glob_mat):
    split_mat = glob_mat.reshape(MATRIX_ROWS, LOCAL_BLOCKS, COL_PROCS, BLOCK_COLS)
    return split_mat.transpose(0, 2, 1, 3).reshape(MATRIX_ROWS, TOTAL_BLOCKS, BLOCK_COLS)


def to_global(stored_mat):
    split_mat = stored_mat.reshape(MATRIX_ROWS, COL_PROCS, LOCAL_BLOCKS, BLOCK_COLS)
    return split_mat.transpose(0, 2, 1, 3).reshape(MATRIX_ROWS, MATRIX_COLS)


def setup_inputs(seed: int = 0, part: int = 0) -> dict:
    base_key = jax.random.fold_in(jax.random.key(seed), part)
    key_gauss, key_left, key_right, key_sign = jax.random.split(base_key, 4)
    gauss_part = jax.random.normal(key_gauss, (MATRIX_ROWS, MATRIX_COLS), jnp.float32)
    low_left = jax.random.normal(key_left, (MATRIX_ROWS, 4), jnp.float32)
    low_right = 0.35 * jax.random.normal(key_right, (4, MATRIX_COLS), jnp.float32)
    pivot_sign = 2.0 * jax.random.randint(key_sign, (PANEL_COLS,), 0, 2).astype(jnp.float32) - 1.0
    dense_mat = gauss_part + mat_dot(low_left, low_right)
    diag_ids = jnp.arange(PANEL_COLS)
    dense_mat = dense_mat.at[diag_ids, diag_ids].add(1.2 * math.sqrt(MATRIX_ROWS) * pivot_sign)
    return {'mat_blocks': to_stored(dense_mat)}


def factor_panel(panel_in, pivot_base):
    row_ids = jnp.arange(MATRIX_ROWS)
    col_ids = jnp.arange(BLOCK_COLS)

    def column_step(col_idx, loop_state):
        panel_work, tau_vec = loop_state
        pivot_row = pivot_base + col_idx
        column = lax.dynamic_index_in_dim(panel_work, col_idx, axis=1, keepdims=False)
        alpha_val = lax.dynamic_index_in_dim(column, pivot_row, keepdims=False)
        sub_col = jnp.where(row_ids > pivot_row, column, 0.0)
        norm_val = jnp.sqrt(alpha_val * alpha_val + jnp.sum(sub_col * sub_col))
        beta_val = jnp.where(alpha_val >= 0.0, -norm_val, norm_val)
        tau_val = (beta_val - alpha_val) / beta_val
        refl_vec = sub_col / (alpha_val - beta_val) + jnp.where(row_ids == pivot_row, 1.0, 0.0)
        refl_dot = mat_dot(refl_vec[None, :], panel_work)[0]
        refl_dot = jnp.where(col_ids > col_idx, refl_dot, 0.0)
        new_col = jnp.where(row_ids < pivot_row, column, jnp.where(row_ids == pivot_row, beta_val, refl_vec))
        panel_work = panel_work - tau_val * refl_vec[:, None] * refl_dot[None, :]
        panel_work = jnp.where(col_ids[None, :] == col_idx, new_col[:, None], panel_work)
        tau_vec = jnp.where(col_ids == col_idx, tau_val, tau_vec)
        return panel_work, tau_vec

    return lax.fori_loop(0, BLOCK_COLS, column_step, (panel_in, jnp.zeros((BLOCK_COLS,), jnp.float32)))


def form_tfactor(refl_mat, tau_vec):
    gram_mat = mat_dot(refl_mat.T, refl_mat)
    col_ids = jnp.arange(BLOCK_COLS)

    def tcol_step(col_idx, t_factor):
        gram_col = lax.dynamic_index_in_dim(gram_mat, col_idx, axis=1, keepdims=False)
        tau_val = lax.dynamic_index_in_dim(tau_vec, col_idx, keepdims=False)
        gram_col = jnp.where(col_ids < col_idx, gram_col, 0.0)
        new_col = -tau_val * mat_dot(t_factor, gram_col[:, None])[:, 0]
        new_col = jnp.where(col_ids == col_idx, tau_val, new_col)
        return jnp.where(col_ids[None, :] == col_idx, new_col[:, None], t_factor)

    return lax.fori_loop(0, BLOCK_COLS, tcol_step, jnp.zeros((BLOCK_COLS, BLOCK_COLS), jnp.float32))


def reference(mat_blocks):
    glob_mat = to_global(mat_blocks)
    row_ids = jnp.arange(MATRIX_ROWS)
    col_ids = jnp.arange(BLOCK_COLS)
    tau_list = []
    tfac_list = []
    for panel_idx in range(PANELS):
        col_start = panel_idx * BLOCK_COLS
        col_end = col_start + BLOCK_COLS
        panel_out, tau_vec = factor_panel(glob_mat[:, col_start:col_end], col_start)
        pivot_ids = col_start + col_ids
        refl_mat = jnp.where(row_ids[:, None] > pivot_ids[None, :], panel_out, jnp.where(row_ids[:, None] == pivot_ids[None, :], 1.0, 0.0))
        t_factor = form_tfactor(refl_mat, tau_vec)
        trail_mat = glob_mat[:, col_end:]
        w_mat = mat_dot(t_factor.T, mat_dot(refl_mat.T, trail_mat))
        trail_mat = trail_mat - mat_dot(refl_mat, w_mat)
        glob_mat = jnp.concatenate([glob_mat[:, :col_start], panel_out, trail_mat], axis=1)
        tau_list.append(tau_vec)
        tfac_list.append(t_factor)
    return to_stored(glob_mat), jnp.concatenate(tau_list), jnp.stack(tfac_list)
```

```python
import functools
import math
import jax
import jax.numpy as jnp
from jax import lax
from jax.experimental import pallas as pl
from jax.experimental.pallas import tpu as pltpu
from jax.sharding import PartitionSpec as P

PANELS = 4
HIGHEST = lax.Precision.HIGHEST
MESH = pl.DeviceIdType.MESH
COND_MAX = 1.0e4
ABS_MAX = 1.0e15
GRAM_MIN = 1.0e-4


def mat_dot(left_mat, right_mat):
    return jnp.dot(left_mat, right_mat, precision=HIGHEST, preferred_element_type=jnp.float32)


def mat_einsum(einsum_form, left_mat, right_mat):
    return jnp.einsum(einsum_form, left_mat, right_mat, precision=HIGHEST, preferred_element_type=jnp.float32)


def axis_sum_kernel(axis, count, x_ref, out_ref, recv_buf, send_sem, recv_sem):
    me = lax.axis_index(axis)
    barrier = pltpu.get_barrier_semaphore()
    for step in range(1, count):
        pl.semaphore_signal(barrier, inc=1, device_id={axis: lax.rem(me + step, count)}, device_id_type=MESH)
    pl.semaphore_wait(barrier, count - 1)

    def copy(step, slot):
        return pltpu.make_async_remote_copy(
            src_ref=x_ref, dst_ref=recv_buf.at[slot], send_sem=send_sem.at[step], recv_sem=recv_sem.at[step],
            device_id={axis: lax.rem(me + step, count)}, device_id_type=MESH)

    for step in range(1, count):
        copy(step, me).start()
    recv_buf[me] = x_ref[...]
    for step in range(1, count):
        copy(step, lax.rem(me + count - step, count)).wait_recv()
    total = recv_buf[0]
    for i in range(1, count):
        total = total + recv_buf[i]
    out_ref[...] = total
    for step in range(1, count):
        copy(step, me).wait_send()


def axis_sum(x, axis, count, collective_id):
    size = math.prod(x.shape)
    lines = -(-size // 1024) * 8
    flat = jnp.pad(x.reshape(-1), (0, lines * 128 - size)).reshape(lines, 128)
    spec = pl.BlockSpec(memory_space=pltpu.VMEM)
    total = pl.pallas_call(
        functools.partial(axis_sum_kernel, axis, count),
        out_shape=jax.ShapeDtypeStruct(flat.shape, jnp.float32),
        in_specs=[spec],
        out_specs=spec,
        scratch_shapes=[pltpu.VMEM((count,) + flat.shape, jnp.float32), pltpu.SemaphoreType.DMA((count,)), pltpu.SemaphoreType.DMA((count,))],
        compiler_params=pltpu.CompilerParams(collective_id=collective_id, has_side_effects=True),
        name='axis_sum',
    )(flat)
    return total.reshape(-1)[:size].reshape(x.shape)


def apply_reflector(panel_work, tau_vec, column, col_idx, pivot_row, row_ids, tail_dots, pivot_line):
    col_ids = jnp.arange(panel_work.shape[1])
    alpha_val = lax.dynamic_index_in_dim(pivot_line, col_idx, keepdims=False)
    norm_val = jnp.sqrt(lax.dynamic_index_in_dim(tail_dots, col_idx, keepdims=False))
    beta_val = jnp.where(alpha_val >= 0.0, -norm_val, norm_val)
    tau_val = (beta_val - alpha_val) / beta_val
    scale_val = 1.0 / (alpha_val - beta_val)
    refl_vec = jnp.where(row_ids > pivot_row, column * scale_val, jnp.where(row_ids == pivot_row, 1.0, 0.0))
    refl_dot = scale_val * (tail_dots - alpha_val * pivot_line) + pivot_line
    refl_dot = jnp.where(col_ids > col_idx, refl_dot, 0.0)
    new_col = jnp.where(row_ids < pivot_row, column, jnp.where(row_ids == pivot_row, beta_val, refl_vec))
    panel_work = jnp.where(col_ids[None, :] == col_idx, new_col[:, None], panel_work - tau_val * refl_vec[:, None] * refl_dot[None, :])
    tau_vec = jnp.where(col_ids == col_idx, tau_val, tau_vec)
    return panel_work, tau_vec


def factor_panel_rows(panel_in, row_base, pivot_base, row_count):
    local_rows, block_width = panel_in.shape
    row_ids = row_base + jnp.arange(local_rows)

    def column_step(col_idx, loop_state):
        panel_work, tau_vec = loop_state
        pivot_row = pivot_base + col_idx
        column = lax.dynamic_index_in_dim(panel_work, col_idx, axis=1, keepdims=False)
        tail_col = jnp.where(row_ids >= pivot_row, column, 0.0)
        local_pivot = jnp.clip(pivot_row - row_base, 0, local_rows - 1)
        holds_pivot = (pivot_row >= row_base) & (pivot_row < row_base + local_rows)
        pivot_line = lax.dynamic_index_in_dim(panel_work, local_pivot, axis=0, keepdims=False)
        pivot_line = jnp.where(holds_pivot, pivot_line, 0.0)
        packed = jnp.concatenate([mat_dot(tail_col[None, :], panel_work)[0], pivot_line])
        packed = axis_sum(packed, 'row', row_count, 1)
        return apply_reflector(panel_work, tau_vec, column, col_idx, pivot_row, row_ids, packed[:block_width], packed[block_width:])

    return lax.fori_loop(0, block_width, column_step, (panel_in, jnp.zeros((block_width,), jnp.float32)))


def tfactor_from_gram(gram_mat, tau_vec):
    block_width = gram_mat.shape[0]
    col_ids = jnp.arange(block_width)
    step_mat = -tau_vec[:, None] * jnp.where(col_ids[None, :] > col_ids[:, None], gram_mat, 0.0)
    eye_mat = jnp.eye(block_width, dtype=jnp.float32)
    inv_acc = eye_mat + step_mat
    power_mat = step_mat
    for _ in range(max(1, math.ceil(math.log2(block_width))) - 1):
        power_mat = mat_dot(power_mat, power_mat)
        inv_acc = mat_dot(inv_acc, eye_mat + power_mat)
    return inv_acc * tau_vec[None, :]


def columnwise_qr(a_local, col_count, row_count):
    local_rows, local_blocks, block_width = a_local.shape
    col_rank = lax.axis_index('col')
    row_base = lax.axis_index('row') * local_rows
    row_ids = row_base + jnp.arange(local_rows)
    col_ids = jnp.arange(block_width)
    global_ids = jnp.arange(local_blocks) * col_count + col_rank

    def panel_step(panel_idx, loop_state):
        a_local, tau_out, tfac_out = loop_state
        owner_col = panel_idx % col_count
        pivot_ids = panel_idx * block_width + col_ids
        panel_in = lax.dynamic_index_in_dim(a_local, panel_idx // col_count, axis=1, keepdims=False)
        panel_out, tau_vec = factor_panel_rows(panel_in, row_base, panel_idx * block_width, row_count)
        refl_mat = jnp.where(row_ids[:, None] > pivot_ids[None, :], panel_out, jnp.where(row_ids[:, None] == pivot_ids[None, :], 1.0, 0.0))
        gram_mat = axis_sum(mat_einsum('rk,rj->kj', refl_mat, refl_mat), 'row', row_count, 2)
        t_factor = tfactor_from_gram(gram_mat, tau_vec)
        packed = jnp.concatenate([refl_mat, t_factor], axis=0)
        packed = axis_sum(jnp.where(col_rank == owner_col, packed, 0.0), 'col', col_count, 3)
        refl_mat = packed[:local_rows]
        t_factor = packed[local_rows:]
        w_summed = axis_sum(mat_einsum('rk,rbc->kbc', refl_mat, a_local), 'row', row_count, 4)
        w_mat = mat_einsum('kj,kbc->jbc', t_factor, w_summed)
        w_mat = jnp.where((global_ids > panel_idx)[None, :, None], w_mat, 0.0)
        a_local = a_local - mat_einsum('rj,jbc->rbc', refl_mat, w_mat)
        a_local = jnp.where((global_ids == panel_idx)[None, :, None], panel_out[:, None, :], a_local)
        tau_out = lax.dynamic_update_index_in_dim(tau_out, jnp.diagonal(t_factor), panel_idx, 0)
        tfac_out = lax.dynamic_update_index_in_dim(tfac_out, t_factor, panel_idx, 0)
        return a_local, tau_out, tfac_out

    zero_tau = jnp.zeros((PANELS, block_width), jnp.float32)
    zero_tfac = jnp.zeros((PANELS, block_width, block_width), jnp.float32)
    a_local, tau_out, tfac_out = lax.fori_loop(0, PANELS, panel_step, (a_local, zero_tau, zero_tfac))
    return a_local, tau_out.reshape(-1), tfac_out


CHUNKS = 8
CROSS_ROWS = 256


def dot_nn(left_mat, right_mat):
    return lax.dot_general(left_mat, right_mat, (((1,), (0,)), ((), ())), precision=HIGHEST, preferred_element_type=jnp.float32)


def split3(mat):
    hi = mat.astype(jnp.bfloat16)
    rest = mat - hi.astype(jnp.float32)
    mid = rest.astype(jnp.bfloat16)
    return hi, mid, (rest - mid.astype(jnp.float32)).astype(jnp.bfloat16)


def bf_nn(left_mat, right_mat):
    return lax.dot_general(left_mat, right_mat, (((1,), (0,)), ((), ())), preferred_element_type=jnp.float32)


def bf_nt(left_mat, right_mat):
    return lax.dot_general(left_mat, right_mat, (((1,), (1,)), ((), ())), preferred_element_type=jnp.float32)


def dot_nt(left_mat, right_mat):
    return lax.dot_general(left_mat, right_mat, (((1,), (1,)), ((), ())), precision=HIGHEST, preferred_element_type=jnp.float32)


def factor_steps(w_ref, vinv_ref, rv_ref, u_ref):
    n = vinv_ref.shape[0]
    row_ids = lax.broadcasted_iota(jnp.int32, (n, n), 0)
    lane_ids = lax.broadcasted_iota(jnp.int32, (n, n), 1)
    line_ids = lax.broadcasted_iota(jnp.int32, (1, n), 1)

    def step(k, tau_line):
        g_line = w_ref[pl.ds(2 * n + k, 1), :]
        m_line = w_ref[pl.ds(k, 1), :]
        here = line_ids == k
        norm_sq = jnp.sum(jnp.where(here, g_line, 0.0), axis=1, keepdims=True)
        alpha = jnp.sum(jnp.where(here, m_line, 0.0), axis=1, keepdims=True)
        norm = jnp.sqrt(norm_sq)
        beta = jnp.where(alpha >= 0.0, -norm, norm)
        pivot = alpha - beta
        beta_rec = 1.0 / beta
        pivot_rec = 1.0 / pivot
        tau_line = jnp.where(here, (beta - alpha) * beta_rec, tau_line)
        r_line = jnp.where(here, beta, jnp.where(line_ids > k, g_line * beta_rec, 0.0))
        u_line = jnp.where(line_ids >= k, m_line - r_line, 0.0)
        u_ref[pl.ds(k, 1), :] = u_line
        v_line = vinv_ref[pl.ds(k, 1), :]
        u_tail = jnp.where(line_ids > k, u_line, 0.0)
        r_tail = jnp.where(line_ids > k, r_line, 0.0)
        at_col = lane_ids == k
        col_m = jnp.sum(jnp.where(at_col, w_ref[0:n], 0.0), axis=1, keepdims=True) * pivot_rec
        col_u = jnp.sum(jnp.where(at_col, w_ref[n:2 * n], 0.0), axis=1, keepdims=True) * pivot_rec
        col_g = jnp.sum(jnp.where(at_col, w_ref[2 * n:3 * n], 0.0), axis=1, keepdims=True) * beta_rec
        col_r = jnp.sum(jnp.where(at_col, w_ref[3 * n:4 * n], 0.0), axis=1, keepdims=True) * beta_rec
        col_m = jnp.where(row_ids[:, 0:1] > k, col_m, 0.0)
        col_g = jnp.where(row_ids[:, 0:1] > k, col_g, 0.0)
        rv_ref[...] = jnp.where(at_col & (row_ids > k), col_m, rv_ref[...])
        rv_ref[pl.ds(k, 1), :] = rv_ref[pl.ds(k, 1), :] + r_line
        w_ref[0:n] = w_ref[0:n] - col_m * u_tail
        w_ref[n:2 * n] = jnp.where(at_col, col_u, w_ref[n:2 * n] - col_u * u_tail)
        w_ref[2 * n:3 * n] = w_ref[2 * n:3 * n] - col_g * r_tail
        w_ref[3 * n:4 * n] = jnp.where(at_col, col_r, w_ref[3 * n:4 * n] - col_r * r_tail)
        vinv_ref[...] = vinv_ref[...] - col_m * v_line
        return tau_line

    return lax.fori_loop(0, n, step, jnp.zeros((1, n), jnp.float32))


def front_kernel(row_count, block_width, a_hbm, a_copy, vt_out, yt_out, rvt_out, tau_out, tf_out, flag_out,
                 a_buf, lead, ct_acc, g_acc, g_send, g_recv, g_part, g_all, c_recv, top_t, a11_t, yt_buf, max_buf,
                 w_ref, vinv_ref, rv_ref, u_ref,
                 own_sem, load_sem, keep_sem, right_send, left_send, fwd_send, from_left, from_right, fwd_recv,
                 max_send, max_recv, a11_send, a11_recv, top_send, top_recv,
                 gs_send, gs_recv, ga_send, ga_recv, cs_send, cs_recv, y_send, y_recv):
    local_cols, local_rows = a_hbm.shape
    n = PANELS * block_width
    chunk = local_rows // CHUNKS
    share = local_cols // row_count
    g_rows = n // row_count
    row_rank = lax.axis_index('row')
    col_rank = lax.axis_index('col')
    right_col, left_col, far_col = lax.rem(col_rank + 1, 4), lax.rem(col_rank + 3, 4), lax.rem(col_rank + 2, 4)

    def lanes(c):
        return pl.ds(pl.multiple_of(c * chunk, chunk), chunk)

    def panel(p):
        return pl.ds(pl.multiple_of(p * block_width, block_width), block_width)

    def peer_of(step):
        return lax.rem(row_rank + step, row_count)

    def own_copy(c):
        return pltpu.make_async_copy(a_hbm.at[0:block_width, lanes(c)], lead.at[panel(col_rank), lanes(c)], own_sem.at[c])

    def load_copy(c):
        return pltpu.make_async_copy(a_hbm.at[:, lanes(c)], a_buf.at[:, lanes(c)], load_sem.at[c])

    def keep_copy(c):
        return pltpu.make_async_copy(a_buf.at[:, lanes(c)], a_copy.at[:, lanes(c)], keep_sem.at[c])

    def to_col(c, owner, target, send_sem, recv_sem):
        return pltpu.make_async_remote_copy(
            src_ref=lead.at[panel(owner), lanes(c)], dst_ref=lead.at[panel(owner), lanes(c)],
            send_sem=send_sem.at[c], recv_sem=recv_sem.at[c], device_id={'col': target}, device_id_type=MESH)

    def to_row(src_ref, dst_ref, send_sem, recv_sem, target):
        return pltpu.make_async_remote_copy(
            src_ref=src_ref, dst_ref=dst_ref, send_sem=send_sem, recv_sem=recv_sem,
            device_id={'row': target}, device_id_type=MESH)

    def send_right(c):
        return to_col(c, col_rank, right_col, right_send, from_left)

    def send_left(c):
        return to_col(c, col_rank, left_col, left_send, from_right)

    @pl.loop(0, CHUNKS)
    def _(c):
        own_copy(c).start()

    @pl.loop(0, CHUNKS)
    def _(c):
        load_copy(c).start()

    barrier = pltpu.get_barrier_semaphore()
    for step in range(1, row_count):
        pl.semaphore_signal(barrier, inc=1, device_id={'row': peer_of(step)}, device_id_type=MESH)
    for step in range(1, 4):
        pl.semaphore_signal(barrier, inc=1, device_id={'col': lax.rem(col_rank + step, 4)}, device_id_type=MESH)
    pl.semaphore_wait(barrier, row_count - 1 + 3)

    def top_copy(target):
        return to_row(a_hbm.at[pl.ds(pl.multiple_of(target * share, share), share), 0:n], top_t, top_send.at[target], top_recv, target)

    def a11_copy(target):
        return to_row(lead.at[:, 0:n], a11_t, a11_send.at[target], a11_recv, target)

    for c in range(2):
        own_copy(c).wait()
        send_right(c).start()
        send_left(c).start()
    g_acc[...] = jnp.zeros_like(g_acc)
    ct_acc[...] = jnp.zeros_like(ct_acc)

    def cross_step(c):
        hi, mid, lo = split3(lead[:, lanes(c)])
        hi_mid = jnp.concatenate([hi, mid], axis=0)

        @pl.loop(0, local_cols // CROSS_ROWS)
        def _(i):
            at_rows = pl.ds(pl.multiple_of(i * CROSS_ROWS, CROSS_ROWS), CROSS_ROWS)
            a_hi, a_mid, a_lo = split3(a_buf[at_rows, lanes(c)])
            pair = bf_nt(a_mid, hi_mid) + bf_nt(a_hi, hi_mid)
            rest = bf_nt(a_lo, hi) + bf_nt(a_hi, lo)
            ct_acc[at_rows, :] = ct_acc[at_rows, :] + (pair[:, 0:n] + (pair[:, n:] + rest))

    def abs_max(c):
        part = jnp.abs(a_buf[:, lanes(c)])
        return jnp.max(jnp.max(part.reshape(local_cols // 8, 8, chunk), axis=0).reshape(8, chunk // 128, 128), axis=1)

    def max_copy(step):
        target = lax.rem(col_rank + step, 4)
        return pltpu.make_async_remote_copy(
            src_ref=max_buf.at[0], dst_ref=max_buf.at[step], send_sem=max_send.at[step], recv_sem=max_recv.at[step],
            device_id={'col': target}, device_id_type=MESH)

    max_buf[0] = jnp.zeros((8, 128), jnp.float32)

    @pl.loop(0, CHUNKS + 1)
    def _(c):
        @pl.when(c + 2 < CHUNKS)
        def _():
            own_copy(c + 2).wait()
            send_right(c + 2).start()
            send_left(c + 2).start()

        @pl.when(c < CHUNKS)
        def _():
            to_col(c, left_col, right_col, right_send, from_left).wait_recv()
            to_col(c, right_col, left_col, left_send, from_right).wait_recv()

            @pl.when(lax.rem(c, 2) == 0)
            def _():
                to_col(c, left_col, right_col, fwd_send, fwd_recv).start()

            @pl.when(lax.rem(c, 2) == 1)
            def _():
                to_col(c, right_col, left_col, fwd_send, fwd_recv).start()
            load_copy(c).wait()
            keep_copy(c).start()
            max_buf[0] = jnp.maximum(max_buf[0], abs_max(c))

        @pl.when(c > 0)
        def _():
            to_col(c - 1, far_col, right_col, fwd_send, fwd_recv).wait_recv()
            part = lead[:, lanes(c - 1)]
            g_acc[...] = g_acc[...] + dot_nt(part, part)

        @pl.when(c == 1)
        def _():
            @pl.when(row_rank == 0)
            def _():
                for target in range(1, row_count):
                    top_copy(target).start()
                    a11_copy(target).start()

        @pl.when(c == CHUNKS - 1)
        def _():
            for step in range(1, 4):
                max_copy(step).start()

        @pl.when(c > CHUNKS // 2)
        def _():
            cross_step(c - CHUNKS // 2 - 1)

    for step in range(1, 4):
        max_copy(step).wait_recv()
    big = jnp.maximum(jnp.maximum(max_buf[0], max_buf[1]), jnp.maximum(max_buf[2], max_buf[3]))
    for i in range(row_count):
        g_send[i, 0:g_rows] = g_acc[i * g_rows:(i + 1) * g_rows, :]
        g_send[i, g_rows:g_rows + 8] = big

    def gs_copy(step):
        return to_row(g_send.at[peer_of(step)], g_recv.at[row_rank], gs_send.at[step], gs_recv.at[step], peer_of(step))

    def ga_copy(step):
        return to_row(g_part, g_all.at[row_rank], ga_send.at[step], ga_recv.at[step], peer_of(step))

    def cs_copy(step):
        at_rows = pl.ds(pl.multiple_of(peer_of(step) * share, share), share)
        return to_row(ct_acc.at[at_rows, :], c_recv.at[row_rank], cs_send.at[step], cs_recv.at[step], peer_of(step))

    my_share = pl.ds(pl.multiple_of(row_rank * share, share), share)

    def y_copy(step):
        return to_row(yt_buf.at[my_share, :], yt_buf.at[my_share, :], y_send.at[step], y_recv.at[step], peer_of(step))

    def arrived(send_kind, buf, sems, step):
        source = lax.rem(row_rank + row_count - step, row_count)
        to_row(buf.at[source], buf.at[source], send_kind.at[step], sems.at[step], source).wait_recv()

    for step in range(1, row_count):
        gs_copy(step).start()
    g_recv[row_rank] = g_send[row_rank]

    @pl.loop(CHUNKS // 2, 3 * CHUNKS // 4)
    def _(c):
        cross_step(c)
    for step in range(1, row_count):
        arrived(gs_send, g_recv, gs_recv, step)
    total = g_recv[0, 0:g_rows]
    big = g_recv[0, g_rows:g_rows + 8]
    for i in range(1, row_count):
        total = total + g_recv[i, 0:g_rows]
        big = jnp.maximum(big, g_recv[i, g_rows:g_rows + 8])
    g_part[0:g_rows] = total
    g_part[g_rows:g_rows + 8] = big
    for step in range(1, row_count):
        ga_copy(step).start()
    g_all[row_rank] = g_part[...]

    @pl.loop(3 * CHUNKS // 4, CHUNKS)
    def _(c):
        cross_step(c)
    for step in range(1, row_count):
        cs_copy(step).start()
    c_recv[row_rank] = ct_acc[my_share, :]
    for step in range(1, row_count):
        arrived(ga_send, g_all, ga_recv, step)

    @pl.when(row_rank == 0)
    def _():
        a11_t[...] = lead[:, 0:n]
        top_t[...] = a_buf[0:share, 0:n]

    @pl.when(row_rank > 0)
    def _():
        a11_copy(row_rank).wait_recv()
        top_copy(row_rank).wait_recv()

    row_ids = lax.broadcasted_iota(jnp.int32, (n, n), 0)
    lane_ids = lax.broadcasted_iota(jnp.int32, (n, n), 1)
    eye = jnp.where(row_ids == lane_ids, 1.0, 0.0)
    big = g_all[0, g_rows:g_rows + 8]
    for i in range(row_count):
        g_acc[i * g_rows:(i + 1) * g_rows, :] = g_all[i, 0:g_rows]
        big = jnp.maximum(big, g_all[i, g_rows:g_rows + 8])
    w_ref[0:n] = a11_t[...].T
    w_ref[n:2 * n] = eye
    w_ref[2 * n:3 * n] = g_acc[...]
    w_ref[3 * n:4 * n] = eye
    vinv_ref[...] = eye
    rv_ref[...] = jnp.zeros((n, n), jnp.float32)
    u_ref[...] = jnp.zeros((n, n), jnp.float32)
    tau_out[...] = factor_steps(w_ref, vinv_ref, rv_ref, u_ref)
    u_inv = w_ref[n:2 * n]
    r_inv = w_ref[3 * n:4 * n]

    for step in range(1, row_count):
        arrived(cs_send, c_recv, cs_recv, step)
    cross = c_recv[0]
    for i in range(1, row_count):
        cross = cross + c_recv[i]
    yt_buf[my_share, :] = dot_nt(top_t[...] - dot_nn(cross, r_inv), vinv_ref[...])
    for step in range(1, row_count):
        y_copy(step).start()

    diag = jnp.sum(jnp.where(row_ids == lane_ids, g_acc[...], 0.0), axis=1, keepdims=True)
    cond_val = jnp.sum(jnp.sum(diag * r_inv * r_inv, axis=1, keepdims=True), axis=0, keepdims=True)
    big_val = jnp.max(jnp.max(big, axis=1, keepdims=True), axis=0, keepdims=True)
    low_val = jnp.min(diag, axis=0, keepdims=True)
    usable = (cond_val < COND_MAX) & (big_val < ABS_MAX) & (low_val > GRAM_MIN)
    flag_out[...] = jnp.broadcast_to(jnp.where(usable, 1.0, 0.0), (8, 128))
    tf_out[...] = -dot_nn(u_ref[...], dot_nt(r_inv, vinv_ref[...]))
    rv_t = rv_ref[...].T
    rvt_out[...] = rv_t
    u_inv_t = u_inv.T

    @pl.loop(0, CHUNKS)
    def _(c):
        vt_out[:, lanes(c)] = dot_nn(u_inv_t, lead[:, lanes(c)])

    @pl.when(row_rank == 0)
    def _():
        vt_out[:, 0:n] = jnp.where(lane_ids > row_ids, rv_t, eye)

    for step in range(1, row_count):
        source = lax.rem(row_rank + row_count - step, row_count)
        at_rows = pl.ds(pl.multiple_of(source * share, share), share)
        to_row(yt_buf.at[at_rows, :], yt_buf.at[at_rows, :], y_send.at[step], y_recv.at[step], source).wait_recv()
    yt_out[...] = yt_buf[...]

    @pl.loop(0, CHUNKS)
    def _(c):
        send_right(c).wait_send()
        send_left(c).wait_send()
        to_col(c, left_col, right_col, fwd_send, fwd_recv).wait_send()
        keep_copy(c).wait()
    for step in range(1, 4):
        max_copy(step).wait_send()
    for step in range(1, row_count):
        gs_copy(step).wait_send()
        ga_copy(step).wait_send()
        cs_copy(step).wait_send()
        y_copy(step).wait_send()

    @pl.when(row_rank == 0)
    def _():
        for target in range(1, row_count):
            top_copy(target).wait_send()
            a11_copy(target).wait_send()


def front(a_t, row_count, block_width):
    local_cols, local_rows = a_t.shape
    n = PANELS * block_width
    share = local_cols // row_count
    g_rows = n // row_count
    f32 = jnp.float32
    mat = jax.ShapeDtypeStruct((n, n), f32)
    vmem, sem = pltpu.VMEM, pltpu.SemaphoreType.DMA
    spec = pl.BlockSpec(memory_space=pltpu.VMEM)
    return pl.pallas_call(
        functools.partial(front_kernel, row_count, block_width),
        out_shape=(jax.ShapeDtypeStruct(a_t.shape, f32), jax.ShapeDtypeStruct((n, local_rows), f32), jax.ShapeDtypeStruct((local_cols, n), f32), mat,
                   jax.ShapeDtypeStruct((1, n), f32), mat, jax.ShapeDtypeStruct((8, 128), f32)),
        in_specs=[pl.BlockSpec(memory_space=pl.ANY)],
        out_specs=[pl.BlockSpec(memory_space=pl.ANY)] + [spec] * 6,
        scratch_shapes=[
            vmem((local_cols, local_rows), f32), vmem((n, local_rows), f32), vmem((local_cols, n), f32), vmem((n, n), f32),
            vmem((row_count, g_rows + 8, n), f32), vmem((row_count, g_rows + 8, n), f32), vmem((g_rows + 8, n), f32),
            vmem((row_count, g_rows + 8, n), f32), vmem((row_count, share, n), f32), vmem((share, n), f32), vmem((n, n), f32),
            vmem((local_cols, n), f32), vmem((4, 8, 128), f32),
            vmem((4 * n, n), f32), vmem((n, n), f32), vmem((n, n), f32), vmem((n, n), f32),
            sem((CHUNKS,)), sem((CHUNKS,)), sem((CHUNKS,)), sem((CHUNKS,)), sem((CHUNKS,)), sem((CHUNKS,)), sem((CHUNKS,)), sem((CHUNKS,)), sem((CHUNKS,)),
            sem((4,)), sem((4,)), sem((row_count,)), sem, sem((row_count,)), sem,
            sem((row_count,)), sem((row_count,)), sem((row_count,)), sem((row_count,)),
            sem((row_count,)), sem((row_count,)), sem((row_count,)), sem((row_count,)),
        ],
        compiler_params=pltpu.CompilerParams(collective_id=0, has_side_effects=True, vmem_limit_bytes=60 * 1024 * 1024),
        name='front',
    )(a_t)


def update_kernel(block_width, a_ref, vt_ref, yt_ref, rvt_ref, out_ref, y_hm, y_hl):
    n = vt_ref.shape[0]
    local_cols = a_ref.shape[0]
    step_rows = 256
    own = pl.ds(pl.multiple_of(lax.axis_index('col') * block_width, block_width), block_width)

    def rows_of(i):
        return pl.ds(pl.multiple_of(i * step_rows, step_rows), step_rows)

    @pl.when(pl.program_id(0) == 0)
    def _():
        @pl.loop(0, local_cols // step_rows)
        def _(i):
            hi, mid, lo = split3(yt_ref[rows_of(i), :])
            y_hm[rows_of(i), :] = jnp.concatenate([hi, mid], axis=1)
            y_hl[rows_of(i), :] = jnp.concatenate([hi, lo], axis=1)

    hi, mid, lo = split3(vt_ref[...])
    hi_hi = jnp.concatenate([hi, hi], axis=0)
    mid_mid = jnp.concatenate([mid, mid], axis=0)
    lo_hi = jnp.concatenate([lo, hi], axis=0)

    @pl.loop(0, local_cols // step_rows)
    def _(i):
        left = y_hm[rows_of(i), :]
        prod = (bf_nn(y_hl[rows_of(i), :], lo_hi) + bf_nn(left, mid_mid)) + bf_nn(left, hi_hi)
        out_ref[rows_of(i), :] = a_ref[rows_of(i), :] - prod
    out_ref[0:block_width, :] = vt_ref[own, :]

    @pl.when((lax.axis_index('row') == 0) & (pl.program_id(0) == 0))
    def _():
        out_ref[0:block_width, 0:n] = rvt_ref[own, :]


def update(a_t, vt, yt, rvt, block_width, tile=512):
    local_cols, local_rows = a_t.shape
    n = vt.shape[0]
    return pl.pallas_call(
        functools.partial(update_kernel, block_width),
        out_shape=jax.ShapeDtypeStruct(a_t.shape, jnp.float32),
        grid=(local_rows // tile,),
        in_specs=[pl.BlockSpec((local_cols, tile), lambda i: (0, i)), pl.BlockSpec((n, tile), lambda i: (0, i)),
                  pl.BlockSpec((local_cols, n), lambda i: (0, 0)), pl.BlockSpec((n, n), lambda i: (0, 0))],
        out_specs=pl.BlockSpec((local_cols, tile), lambda i: (0, i)),
        scratch_shapes=[pltpu.VMEM((local_cols, 2 * n), jnp.bfloat16)] * 2,
        compiler_params=pltpu.CompilerParams(dimension_semantics=('arbitrary',), vmem_limit_bytes=56 * 1024 * 1024),
        name='update',
    )(a_t, vt, yt, rvt)


def solution(mesh):
    col_count = mesh.shape['col']
    row_count = mesh.shape['row']
    assert col_count == PANELS == 4
    block_spec = P(('batch', 'row'), 'col', None)

    def device_fn(a_local):
        local_rows, local_blocks, block_width = a_local.shape
        width = PANELS * block_width
        local_cols = local_blocks * block_width
        a_t = a_local.transpose(1, 2, 0).reshape(local_cols, local_rows)
        kept, vt, yt, rvt, tau_line, t_full, flag = front(a_t, row_count, block_width)
        out_t = update(a_t, vt, yt, rvt, block_width)
        tfac = jnp.stack([t_full[s:s + block_width, s:s + block_width] for s in range(0, width, block_width)])

        def column_form(state):
            kept = state[4]
            a_local = kept.reshape(local_blocks, block_width, local_rows).transpose(2, 0, 1)
            a_out, tau, tfac = columnwise_qr(a_local, col_count, row_count)
            return jnp.int32(0), a_out.transpose(1, 2, 0).reshape(local_cols, local_rows), tau, tfac, kept

        redo = jnp.where(flag[0, 0] > 0.5, 0, 1).astype(jnp.int32)
        state = (redo, out_t, tau_line[0], tfac, kept)
        _, out_t, tau, tfac, _ = lax.while_loop(lambda state: state[0] > 0, column_form, state)
        return out_t.reshape(local_blocks, block_width, local_rows).transpose(2, 0, 1), tau, tfac

    return jax.shard_map(device_fn, mesh=mesh, in_specs=(block_spec,), out_specs=(block_spec, P('batch'), P('batch', None, None)), check_vma=False)
```

```python
import functools
import math
import jax
import jax.numpy as jnp
from jax import lax
from jax.experimental import pallas as pl
from jax.experimental.pallas import tpu as pltpu
from jax.sharding import PartitionSpec as P

PANELS = 4
HIGHEST = lax.Precision.HIGHEST
MESH = pl.DeviceIdType.MESH
COND_MAX = 1.0e4
ABS_MAX = 1.0e15
GRAM_MIN = 1.0e-4


def mat_dot(left_mat, right_mat):
    return jnp.dot(left_mat, right_mat, precision=HIGHEST, preferred_element_type=jnp.float32)


def mat_einsum(einsum_form, left_mat, right_mat):
    return jnp.einsum(einsum_form, left_mat, right_mat, precision=HIGHEST, preferred_element_type=jnp.float32)


def axis_sum_kernel(axis, count, x_ref, out_ref, recv_buf, send_sem, recv_sem):
    me = lax.axis_index(axis)
    barrier = pltpu.get_barrier_semaphore()
    for step in range(1, count):
        pl.semaphore_signal(barrier, inc=1, device_id={axis: lax.rem(me + step, count)}, device_id_type=MESH)
    pl.semaphore_wait(barrier, count - 1)

    def copy(step, slot):
        return pltpu.make_async_remote_copy(
            src_ref=x_ref, dst_ref=recv_buf.at[slot], send_sem=send_sem.at[step], recv_sem=recv_sem.at[step],
            device_id={axis: lax.rem(me + step, count)}, device_id_type=MESH)

    for step in range(1, count):
        copy(step, me).start()
    recv_buf[me] = x_ref[...]
    for step in range(1, count):
        copy(step, lax.rem(me + count - step, count)).wait_recv()
    total = recv_buf[0]
    for i in range(1, count):
        total = total + recv_buf[i]
    out_ref[...] = total
    for step in range(1, count):
        copy(step, me).wait_send()


def axis_sum(x, axis, count, collective_id):
    size = math.prod(x.shape)
    lines = -(-size // 1024) * 8
    flat = jnp.pad(x.reshape(-1), (0, lines * 128 - size)).reshape(lines, 128)
    spec = pl.BlockSpec(memory_space=pltpu.VMEM)
    total = pl.pallas_call(
        functools.partial(axis_sum_kernel, axis, count),
        out_shape=jax.ShapeDtypeStruct(flat.shape, jnp.float32),
        in_specs=[spec],
        out_specs=spec,
        scratch_shapes=[pltpu.VMEM((count,) + flat.shape, jnp.float32), pltpu.SemaphoreType.DMA((count,)), pltpu.SemaphoreType.DMA((count,))],
        compiler_params=pltpu.CompilerParams(collective_id=collective_id, has_side_effects=True),
        name='axis_sum',
    )(flat)
    return total.reshape(-1)[:size].reshape(x.shape)


def apply_reflector(panel_work, tau_vec, column, col_idx, pivot_row, row_ids, tail_dots, pivot_line):
    col_ids = jnp.arange(panel_work.shape[1])
    alpha_val = lax.dynamic_index_in_dim(pivot_line, col_idx, keepdims=False)
    norm_val = jnp.sqrt(lax.dynamic_index_in_dim(tail_dots, col_idx, keepdims=False))
    beta_val = jnp.where(alpha_val >= 0.0, -norm_val, norm_val)
    tau_val = (beta_val - alpha_val) / beta_val
    scale_val = 1.0 / (alpha_val - beta_val)
    refl_vec = jnp.where(row_ids > pivot_row, column * scale_val, jnp.where(row_ids == pivot_row, 1.0, 0.0))
    refl_dot = scale_val * (tail_dots - alpha_val * pivot_line) + pivot_line
    refl_dot = jnp.where(col_ids > col_idx, refl_dot, 0.0)
    new_col = jnp.where(row_ids < pivot_row, column, jnp.where(row_ids == pivot_row, beta_val, refl_vec))
    panel_work = jnp.where(col_ids[None, :] == col_idx, new_col[:, None], panel_work - tau_val * refl_vec[:, None] * refl_dot[None, :])
    tau_vec = jnp.where(col_ids == col_idx, tau_val, tau_vec)
    return panel_work, tau_vec


def factor_panel_rows(panel_in, row_base, pivot_base, row_count):
    local_rows, block_width = panel_in.shape
    row_ids = row_base + jnp.arange(local_rows)

    def column_step(col_idx, loop_state):
        panel_work, tau_vec = loop_state
        pivot_row = pivot_base + col_idx
        column = lax.dynamic_index_in_dim(panel_work, col_idx, axis=1, keepdims=False)
        tail_col = jnp.where(row_ids >= pivot_row, column, 0.0)
        local_pivot = jnp.clip(pivot_row - row_base, 0, local_rows - 1)
        holds_pivot = (pivot_row >= row_base) & (pivot_row < row_base + local_rows)
        pivot_line = lax.dynamic_index_in_dim(panel_work, local_pivot, axis=0, keepdims=False)
        pivot_line = jnp.where(holds_pivot, pivot_line, 0.0)
        packed = jnp.concatenate([mat_dot(tail_col[None, :], panel_work)[0], pivot_line])
        packed = axis_sum(packed, 'row', row_count, 1)
        return apply_reflector(panel_work, tau_vec, column, col_idx, pivot_row, row_ids, packed[:block_width], packed[block_width:])

    return lax.fori_loop(0, block_width, column_step, (panel_in, jnp.zeros((block_width,), jnp.float32)))


def tfactor_from_gram(gram_mat, tau_vec):
    block_width = gram_mat.shape[0]
    col_ids = jnp.arange(block_width)
    step_mat = -tau_vec[:, None] * jnp.where(col_ids[None, :] > col_ids[:, None], gram_mat, 0.0)
    eye_mat = jnp.eye(block_width, dtype=jnp.float32)
    inv_acc = eye_mat + step_mat
    power_mat = step_mat
    for _ in range(max(1, math.ceil(math.log2(block_width))) - 1):
        power_mat = mat_dot(power_mat, power_mat)
        inv_acc = mat_dot(inv_acc, eye_mat + power_mat)
    return inv_acc * tau_vec[None, :]


def columnwise_qr(a_local, col_count, row_count):
    local_rows, local_blocks, block_width = a_local.shape
    col_rank = lax.axis_index('col')
    row_base = lax.axis_index('row') * local_rows
    row_ids = row_base + jnp.arange(local_rows)
    col_ids = jnp.arange(block_width)
    global_ids = jnp.arange(local_blocks) * col_count + col_rank

    def panel_step(panel_idx, loop_state):
        a_local, tau_out, tfac_out = loop_state
        owner_col = panel_idx % col_count
        pivot_ids = panel_idx * block_width + col_ids
        panel_in = lax.dynamic_index_in_dim(a_local, panel_idx // col_count, axis=1, keepdims=False)
        panel_out, tau_vec = factor_panel_rows(panel_in, row_base, panel_idx * block_width, row_count)
        refl_mat = jnp.where(row_ids[:, None] > pivot_ids[None, :], panel_out, jnp.where(row_ids[:, None] == pivot_ids[None, :], 1.0, 0.0))
        gram_mat = axis_sum(mat_einsum('rk,rj->kj', refl_mat, refl_mat), 'row', row_count, 2)
        t_factor = tfactor_from_gram(gram_mat, tau_vec)
        packed = jnp.concatenate([refl_mat, t_factor], axis=0)
        packed = axis_sum(jnp.where(col_rank == owner_col, packed, 0.0), 'col', col_count, 3)
        refl_mat = packed[:local_rows]
        t_factor = packed[local_rows:]
        w_summed = axis_sum(mat_einsum('rk,rbc->kbc', refl_mat, a_local), 'row', row_count, 4)
        w_mat = mat_einsum('kj,kbc->jbc', t_factor, w_summed)
        w_mat = jnp.where((global_ids > panel_idx)[None, :, None], w_mat, 0.0)
        a_local = a_local - mat_einsum('rj,jbc->rbc', refl_mat, w_mat)
        a_local = jnp.where((global_ids == panel_idx)[None, :, None], panel_out[:, None, :], a_local)
        tau_out = lax.dynamic_update_index_in_dim(tau_out, jnp.diagonal(t_factor), panel_idx, 0)
        tfac_out = lax.dynamic_update_index_in_dim(tfac_out, t_factor, panel_idx, 0)
        return a_local, tau_out, tfac_out

    zero_tau = jnp.zeros((PANELS, block_width), jnp.float32)
    zero_tfac = jnp.zeros((PANELS, block_width, block_width), jnp.float32)
    a_local, tau_out, tfac_out = lax.fori_loop(0, PANELS, panel_step, (a_local, zero_tau, zero_tfac))
    return a_local, tau_out.reshape(-1), tfac_out


CHUNKS = 4
CROSS_ROWS = 512
SUB = 4
ROWS = 512


def dot_nn(left_mat, right_mat):
    return lax.dot_general(left_mat, right_mat, (((1,), (0,)), ((), ())), precision=HIGHEST, preferred_element_type=jnp.float32)


def split3(mat):
    hi = mat.astype(jnp.bfloat16)
    rest = mat - hi.astype(jnp.float32)
    mid = rest.astype(jnp.bfloat16)
    return hi, mid, (rest - mid.astype(jnp.float32)).astype(jnp.bfloat16)


def bf_nn(left_mat, right_mat):
    return lax.dot_general(left_mat, right_mat, (((1,), (0,)), ((), ())), preferred_element_type=jnp.float32)


def bf_nt(left_mat, right_mat):
    return lax.dot_general(left_mat, right_mat, (((1,), (1,)), ((), ())), preferred_element_type=jnp.float32)


def dot_nt(left_mat, right_mat):
    return lax.dot_general(left_mat, right_mat, (((1,), (1,)), ((), ())), precision=HIGHEST, preferred_element_type=jnp.float32)


def factor_steps(w1_ref, w2_ref, vinv_ref, v_ref, r_ref, u_ref):
    n = vinv_ref.shape[0]
    row_col = lax.broadcasted_iota(jnp.int32, (n, 1), 0)
    lane_ids = lax.broadcasted_iota(jnp.int32, (n, n), 1)
    lane8 = lax.broadcasted_iota(jnp.int32, (8, n), 1)
    sub_col = lax.broadcasted_iota(jnp.int32, (8, 1), 0)
    line_ids = lax.broadcasted_iota(jnp.int32, (1, n), 1)

    def pick(mask, mat):
        return jnp.sum(jnp.where(mask, mat, 0.0), axis=1, keepdims=True)

    def step(b, tau_line):
        base = pl.multiple_of(b * 8, 8)
        rows8 = pl.ds(base, 8)
        for first in range(0, 8, SUB):
            tile1, tile2 = w1_ref[rows8, :], w2_ref[rows8, :]
            ks = [base + first + j for j in range(SUB)]
            d1 = [pick(lane8 == k, tile1) for k in ks]
            d2 = [pick(lane8 == k, tile2) for k in ks]
            w1, w2 = w1_ref[...], w2_ref[...]
            c1 = [pick(lane_ids == k, w1) for k in ks]
            c2 = [pick(lane_ids == k, w2) for k in ks]
            below = row_col >= base + 8
            v_mat = v_ref[...]
            for j in range(SUB):
                at, k = first + j, ks[j]
                alpha, norm_sq = d1[j][at:at + 1], d2[j][at:at + 1]
                norm = jnp.sqrt(norm_sq)
                beta = jnp.where(alpha >= 0.0, -norm, norm)
                beta_rec = 1.0 / beta
                pivot_rec = 1.0 / (alpha - beta)
                line1, line2 = tile1[at:at + 1, :], tile2[at:at + 1, :]
                here, after = line_ids == k, line_ids > k
                tau_line = jnp.where(here, (beta - alpha) * beta_rec, tau_line)
                r_tail = jnp.where(after, line2 * beta_rec, 0.0)
                u_tail = jnp.where(after, line1 - r_tail, 0.0)
                low = jnp.where(line_ids < k, line1, 0.0)
                r_ref[pl.ds(k, 1), :] = jnp.where(here, beta, r_tail)
                u_ref[pl.ds(k, 1), :] = jnp.where(here, alpha - beta, u_tail)
                vinv_ref[pl.ds(k, 1), :] = jnp.where(here, 1.0, low)
                m1 = jnp.where(sub_col == at, pivot_rec, d1[j] * pivot_rec)
                m2 = jnp.where(sub_col == at, beta_rec, d2[j] * beta_rec)
                f1, f2 = c1[j] * pivot_rec, c2[j] * beta_rec
                for t in range(j + 1, SUB):
                    r_val = d2[t][at:at + 1] * beta_rec
                    u_val = d1[t][at:at + 1] - r_val
                    d1[t] = jnp.where(sub_col == at, 0.0, d1[t]) - m1 * u_val
                    d2[t] = jnp.where(sub_col == at, 0.0, d2[t]) - m2 * r_val
                    c1[t] = c1[t] - f1 * u_val
                    c2[t] = c2[t] - f2 * r_val
                here8 = lane8 == k
                rest8 = sub_col > at
                tile1 = jnp.where(here8, jnp.where(rest8, -m1, m1),
                                  jnp.where(sub_col == at, 0.0, tile1) - m1 * jnp.where(rest8, u_tail + low, u_tail))
                tile2 = jnp.where(here8, m2, jnp.where(sub_col == at, 0.0, tile2) - m2 * r_tail)
                v8 = jnp.where(rest8, m1, 0.0)
                at_col = lane_ids == k
                w1 = jnp.where(at_col, jnp.where(below, -f1, f1), w1 - f1 * jnp.where(below, u_tail + low, u_tail))
                w2 = jnp.where(at_col, f2, w2 - f2 * r_tail)
                v_mat = jnp.where(at_col, f1, v_mat)
                v_rows = jnp.where(here8, v8, v_ref[rows8, :] if j == 0 else v_rows)
            w1_ref[...] = w1
            w2_ref[...] = w2
            v_ref[...] = v_mat
            w1_ref[rows8, :] = tile1
            w2_ref[rows8, :] = tile2
            v_ref[rows8, :] = v_rows
        return tau_line

    return lax.fori_loop(0, n // 8, step, jnp.zeros((1, n), jnp.float32))


def front_kernel(row_count, block_width, a_hbm, a_copy, vt_out, yt_out, rvt_out, tau_out, tf_out, flag_out,
                 a_buf, lead, ct_acc, g_acc, g_send, g_recv, g_part, g_all, c_recv, top_t, a11_t, yt_buf, max_buf,
                 w1_ref, w2_ref, vinv_ref, v_ref, r_ref, u_ref,
                 own_sem, load_sem, keep_sem, right_send, left_send, fwd_send, from_left, from_right, fwd_recv,
                 max_send, max_recv, a11_send, a11_recv, top_send, top_recv,
                 gs_send, gs_recv, ga_send, ga_recv, cs_send, cs_recv, y_send, y_recv):
    local_cols, local_rows = a_hbm.shape
    n = PANELS * block_width
    chunk = local_rows // CHUNKS
    share = local_cols // row_count
    g_rows = n // row_count
    row_rank = lax.axis_index('row')
    col_rank = lax.axis_index('col')
    right_col, left_col, far_col = lax.rem(col_rank + 1, 4), lax.rem(col_rank + 3, 4), lax.rem(col_rank + 2, 4)

    def lanes(c):
        return pl.ds(pl.multiple_of(c * chunk, chunk), chunk)

    def panel(p):
        return pl.ds(pl.multiple_of(p * block_width, block_width), block_width)

    def peer_of(step):
        return lax.rem(row_rank + step, row_count)

    def own_copy(c):
        return pltpu.make_async_copy(a_hbm.at[0:block_width, lanes(c)], lead.at[panel(col_rank), lanes(c)], own_sem.at[c])

    def load_copy(c):
        return pltpu.make_async_copy(a_hbm.at[:, lanes(c)], a_buf.at[:, lanes(c)], load_sem.at[c])

    def keep_copy(c):
        return pltpu.make_async_copy(a_buf.at[:, lanes(c)], a_copy.at[:, lanes(c)], keep_sem.at[c])

    def to_col(c, owner, target, send_sem, recv_sem):
        return pltpu.make_async_remote_copy(
            src_ref=lead.at[panel(owner), lanes(c)], dst_ref=lead.at[panel(owner), lanes(c)],
            send_sem=send_sem.at[c], recv_sem=recv_sem.at[c], device_id={'col': target}, device_id_type=MESH)

    def to_row(src_ref, dst_ref, send_sem, recv_sem, target):
        return pltpu.make_async_remote_copy(
            src_ref=src_ref, dst_ref=dst_ref, send_sem=send_sem, recv_sem=recv_sem,
            device_id={'row': target}, device_id_type=MESH)

    def send_right(c):
        return to_col(c, col_rank, right_col, right_send, from_left)

    def send_left(c):
        return to_col(c, col_rank, left_col, left_send, from_right)

    @pl.loop(0, CHUNKS)
    def _(c):
        own_copy(c).start()

    @pl.loop(0, CHUNKS)
    def _(c):
        load_copy(c).start()

    barrier = pltpu.get_barrier_semaphore()
    for step in range(1, row_count):
        pl.semaphore_signal(barrier, inc=1, device_id={'row': peer_of(step)}, device_id_type=MESH)
    for step in range(1, 4):
        pl.semaphore_signal(barrier, inc=1, device_id={'col': lax.rem(col_rank + step, 4)}, device_id_type=MESH)
    pl.semaphore_wait(barrier, row_count - 1 + 3)

    def top_copy(target):
        return to_row(a_hbm.at[pl.ds(pl.multiple_of(target * share, share), share), 0:n], top_t, top_send.at[target], top_recv, target)

    def a11_copy(target):
        return to_row(lead.at[:, 0:n], a11_t, a11_send.at[target], a11_recv, target)

    for c in range(2):
        own_copy(c).wait()
        send_right(c).start()
        send_left(c).start()
    g_acc[...] = jnp.zeros_like(g_acc)
    ct_acc[...] = jnp.zeros_like(ct_acc)

    def cross_step(c):
        hi, mid, lo = split3(lead[:, lanes(c)])
        hi_mid = jnp.concatenate([hi, mid], axis=0)
        hi_mid = jnp.concatenate([hi_mid, hi_mid], axis=1)
        hi_lo = jnp.concatenate([hi, lo], axis=1)

        @pl.loop(0, local_cols // CROSS_ROWS)
        def _(i):
            at_rows = pl.ds(pl.multiple_of(i * CROSS_ROWS, CROSS_ROWS), CROSS_ROWS)
            a_hi, a_mid, a_lo = split3(a_buf[at_rows, lanes(c)])
            pair = bf_nt(jnp.concatenate([a_mid, a_hi], axis=1), hi_mid)
            rest = bf_nt(jnp.concatenate([a_lo, a_hi], axis=1), hi_lo)
            ct_acc[at_rows, :] = ct_acc[at_rows, :] + (pair[:, 0:n] + (pair[:, n:] + rest))

    def abs_max(c):
        part = jnp.abs(a_buf[:, lanes(c)])
        return jnp.max(jnp.max(part.reshape(local_cols // 8, 8, chunk), axis=0).reshape(8, chunk // 128, 128), axis=1)

    def max_copy(step):
        target = lax.rem(col_rank + step, 4)
        return pltpu.make_async_remote_copy(
            src_ref=max_buf.at[0], dst_ref=max_buf.at[step], send_sem=max_send.at[step], recv_sem=max_recv.at[step],
            device_id={'col': target}, device_id_type=MESH)

    max_buf[0] = jnp.zeros((8, 128), jnp.float32)

    @pl.loop(0, CHUNKS + 1)
    def _(c):
        @pl.when(c + 2 < CHUNKS)
        def _():
            own_copy(c + 2).wait()
            send_right(c + 2).start()
            send_left(c + 2).start()

        @pl.when(c < CHUNKS)
        def _():
            to_col(c, left_col, right_col, right_send, from_left).wait_recv()
            to_col(c, right_col, left_col, left_send, from_right).wait_recv()

            @pl.when(lax.rem(c, 2) == 0)
            def _():
                to_col(c, left_col, right_col, fwd_send, fwd_recv).start()

            @pl.when(lax.rem(c, 2) == 1)
            def _():
                to_col(c, right_col, left_col, fwd_send, fwd_recv).start()
            load_copy(c).wait()
            keep_copy(c).start()
            max_buf[0] = jnp.maximum(max_buf[0], abs_max(c))

        @pl.when(c > 0)
        def _():
            to_col(c - 1, far_col, right_col, fwd_send, fwd_recv).wait_recv()
            part = lead[:, lanes(c - 1)]
            g_acc[...] = g_acc[...] + dot_nt(part, part)

        @pl.when(c == 1)
        def _():
            @pl.when(row_rank == 0)
            def _():
                for target in range(1, row_count):
                    top_copy(target).start()
                    a11_copy(target).start()

        @pl.when(c == CHUNKS - 1)
        def _():
            for step in range(1, 4):
                max_copy(step).start()

        @pl.when((c > 0) & (c < CHUNKS))
        def _():
            cross_step(c - 1)

    for step in range(1, 4):
        max_copy(step).wait_recv()
    big = jnp.maximum(jnp.maximum(max_buf[0], max_buf[1]), jnp.maximum(max_buf[2], max_buf[3]))
    for i in range(row_count):
        g_send[i, 0:g_rows] = g_acc[i * g_rows:(i + 1) * g_rows, :]
        g_send[i, g_rows:g_rows + 8] = big

    def gs_copy(step):
        return to_row(g_send.at[peer_of(step)], g_recv.at[row_rank], gs_send.at[step], gs_recv.at[step], peer_of(step))

    def ga_copy(step):
        return to_row(g_part, g_all.at[row_rank], ga_send.at[step], ga_recv.at[step], peer_of(step))

    def cs_copy(step):
        at_rows = pl.ds(pl.multiple_of(peer_of(step) * share, share), share)
        return to_row(ct_acc.at[at_rows, :], c_recv.at[row_rank], cs_send.at[step], cs_recv.at[step], peer_of(step))

    my_share = pl.ds(pl.multiple_of(row_rank * share, share), share)

    partner = row_rank + 1 - 2 * lax.rem(row_rank, 2)

    def y_rows(owner):
        return pl.ds(pl.multiple_of(owner * share, share), share)

    def y_copy(step):
        target = partner if step == 0 else peer_of(step)
        return to_row(yt_buf.at[my_share, :], yt_buf.at[my_share, :], y_send.at[step], y_recv.at[step], target)

    def y_pass(step):
        source = lax.rem(row_rank + row_count - step, row_count)
        return to_row(yt_buf.at[y_rows(source), :], yt_buf.at[y_rows(source), :], y_send.at[step + 1], y_recv.at[step + 1], partner)

    def y_arrive(owner, slot):
        to_row(yt_buf.at[y_rows(owner), :], yt_buf.at[y_rows(owner), :], y_send.at[slot], y_recv.at[slot], partner).wait_recv()

    def arrived(send_kind, buf, sems, step):
        source = lax.rem(row_rank + row_count - step, row_count)
        to_row(buf.at[source], buf.at[source], send_kind.at[step], sems.at[step], source).wait_recv()

    for step in range(1, row_count):
        gs_copy(step).start()
    g_recv[row_rank] = g_send[row_rank]

    cross_step(CHUNKS - 1)
    for step in range(1, row_count):
        arrived(gs_send, g_recv, gs_recv, step)
    total = g_recv[0, 0:g_rows]
    big = g_recv[0, g_rows:g_rows + 8]
    for i in range(1, row_count):
        total = total + g_recv[i, 0:g_rows]
        big = jnp.maximum(big, g_recv[i, g_rows:g_rows + 8])
    g_part[0:g_rows] = total
    g_part[g_rows:g_rows + 8] = big
    for step in range(1, row_count):
        ga_copy(step).start()
    g_all[row_rank] = g_part[...]

    for step in range(1, row_count):
        cs_copy(step).start()
    c_recv[row_rank] = ct_acc[my_share, :]
    for step in range(1, row_count):
        arrived(ga_send, g_all, ga_recv, step)

    @pl.when(row_rank == 0)
    def _():
        a11_t[...] = lead[:, 0:n]
        top_t[...] = a_buf[0:share, 0:n]

    @pl.when(row_rank > 0)
    def _():
        a11_copy(row_rank).wait_recv()
        top_copy(row_rank).wait_recv()

    row_ids = lax.broadcasted_iota(jnp.int32, (n, n), 0)
    lane_ids = lax.broadcasted_iota(jnp.int32, (n, n), 1)
    eye = jnp.where(row_ids == lane_ids, 1.0, 0.0)
    big = g_all[0, g_rows:g_rows + 8]
    for i in range(row_count):
        g_acc[i * g_rows:(i + 1) * g_rows, :] = g_all[i, 0:g_rows]
        big = jnp.maximum(big, g_all[i, g_rows:g_rows + 8])
    w1_ref[...] = a11_t[...].T
    w2_ref[...] = g_acc[...]
    v_ref[...] = jnp.zeros((n, n), jnp.float32)
    tau_out[...] = factor_steps(w1_ref, w2_ref, vinv_ref, v_ref, r_ref, u_ref)
    u_inv = w1_ref[...]
    r_inv = w2_ref[...]

    for step in range(1, row_count):
        arrived(cs_send, c_recv, cs_recv, step)
    cross = c_recv[0]
    for i in range(1, row_count):
        cross = cross + c_recv[i]
    yt_buf[my_share, :] = dot_nt(top_t[...] - dot_nn(cross, r_inv), vinv_ref[...])
    for step in range(0, row_count, 2):
        y_copy(step).start()

    diag = jnp.sum(jnp.where(row_ids == lane_ids, g_acc[...], 0.0), axis=1, keepdims=True)
    cond_val = jnp.sum(jnp.sum(diag * r_inv * r_inv, axis=1, keepdims=True), axis=0, keepdims=True)
    big_val = jnp.max(jnp.max(big, axis=1, keepdims=True), axis=0, keepdims=True)
    low_val = jnp.min(diag, axis=0, keepdims=True)
    usable = (cond_val < COND_MAX) & (big_val < ABS_MAX) & (low_val > GRAM_MIN)
    flag_out[0, 0] = jnp.max(jnp.where(usable, 0, 1))
    t_full = -dot_nn(u_ref[...], dot_nt(r_inv, vinv_ref[...]))
    for p in range(PANELS):
        tf_out[p] = t_full[p * block_width:(p + 1) * block_width, p * block_width:(p + 1) * block_width]
    rv_t = jnp.where(lane_ids < row_ids, v_ref[...], r_ref[...]).T
    rvt_out[...] = rv_t
    u_inv_t = u_inv.T

    @pl.loop(0, CHUNKS)
    def _(c):
        vt_out[:, lanes(c)] = dot_nn(u_inv_t, lead[:, lanes(c)])

    @pl.when(row_rank == 0)
    def _():
        vt_out[:, 0:n] = jnp.where(lane_ids > row_ids, rv_t, eye)

    for step in range(2, row_count, 2):
        y_arrive(lax.rem(row_rank + row_count - step, row_count), step)
        y_pass(step).start()
    y_arrive(partner, 0)
    for step in range(2, row_count, 2):
        y_arrive(lax.rem(partner + row_count - step, row_count), step + 1)
    yt_out[...] = yt_buf[...]

    @pl.loop(0, CHUNKS)
    def _(c):
        send_right(c).wait_send()
        send_left(c).wait_send()
        to_col(c, left_col, right_col, fwd_send, fwd_recv).wait_send()
        keep_copy(c).wait()
    for step in range(1, 4):
        max_copy(step).wait_send()
    for step in range(1, row_count):
        gs_copy(step).wait_send()
        ga_copy(step).wait_send()
        cs_copy(step).wait_send()
    y_copy(0).wait_send()
    for step in range(2, row_count, 2):
        y_copy(step).wait_send()
        y_pass(step).wait_send()

    @pl.when(row_rank == 0)
    def _():
        for target in range(1, row_count):
            top_copy(target).wait_send()
            a11_copy(target).wait_send()


def front(a_t, row_count, block_width):
    local_cols, local_rows = a_t.shape
    n = PANELS * block_width
    share = local_cols // row_count
    g_rows = n // row_count
    f32 = jnp.float32
    mat = jax.ShapeDtypeStruct((n, n), f32)
    vmem, sem = pltpu.VMEM, pltpu.SemaphoreType.DMA
    spec = pl.BlockSpec(memory_space=pltpu.VMEM)
    return pl.pallas_call(
        functools.partial(front_kernel, row_count, block_width),
        out_shape=(jax.ShapeDtypeStruct(a_t.shape, f32), jax.ShapeDtypeStruct((n, local_rows), f32), jax.ShapeDtypeStruct((local_cols, n), f32), mat,
                   jax.ShapeDtypeStruct((1, n), f32), jax.ShapeDtypeStruct((PANELS, block_width, block_width), f32),
                   jax.ShapeDtypeStruct((1, 1), jnp.int32)),
        in_specs=[pl.BlockSpec(memory_space=pl.ANY)],
        out_specs=[pl.BlockSpec(memory_space=pl.ANY)] + [spec] * 5 + [pl.BlockSpec(memory_space=pltpu.SMEM)],
        scratch_shapes=[
            vmem((local_cols, local_rows), f32), vmem((n, local_rows), f32), vmem((local_cols, n), f32), vmem((n, n), f32),
            vmem((row_count, g_rows + 8, n), f32), vmem((row_count, g_rows + 8, n), f32), vmem((g_rows + 8, n), f32),
            vmem((row_count, g_rows + 8, n), f32), vmem((row_count, share, n), f32), vmem((share, n), f32), vmem((n, n), f32),
            vmem((local_cols, n), f32), vmem((4, 8, 128), f32),
            vmem((n, n), f32), vmem((n, n), f32), vmem((n, n), f32), vmem((n, n), f32), vmem((n, n), f32), vmem((n, n), f32),
            sem((CHUNKS,)), sem((CHUNKS,)), sem((CHUNKS,)), sem((CHUNKS,)), sem((CHUNKS,)), sem((CHUNKS,)), sem((CHUNKS,)), sem((CHUNKS,)), sem((CHUNKS,)),
            sem((4,)), sem((4,)), sem((row_count,)), sem, sem((row_count,)), sem,
            sem((row_count,)), sem((row_count,)), sem((row_count,)), sem((row_count,)),
            sem((row_count,)), sem((row_count,)), sem((row_count,)), sem((row_count,)),
        ],
        compiler_params=pltpu.CompilerParams(collective_id=0, has_side_effects=True, vmem_limit_bytes=60 * 1024 * 1024),
        name='front',
    )(a_t)


def update_kernel(block_width, a_ref, vt_ref, yt_ref, rvt_ref, tau_ref, tf_ref, out_ref, tau_out, tf_out, y_parts):
    n, tile = vt_ref.shape
    local_cols = a_ref.shape[0]
    own = pl.ds(pl.multiple_of(lax.axis_index('col') * block_width, block_width), block_width)

    @pl.when(pl.program_id(0) == 0)
    def _():
        tau_out[...] = tau_ref[...]
        tf_out[...] = tf_ref[...]
        for first in range(0, local_cols, ROWS):
            hi, mid, lo = split3(yt_ref[first:first + ROWS, :])
            y_parts[first:first + ROWS, :] = jnp.concatenate([hi, lo, mid, mid, hi, hi], axis=1)

    for lane in range(0, tile, ROWS):
        hi, mid, lo = split3(vt_ref[:, lane:lane + ROWS])
        vt_parts = jnp.concatenate([lo, hi, mid, hi, mid, hi], axis=0)
        for first in range(0, local_cols, ROWS):
            prod = bf_nn(y_parts[first:first + ROWS, :], vt_parts)
            out_ref[first:first + ROWS, lane:lane + ROWS] = a_ref[first:first + ROWS, lane:lane + ROWS] - prod
    out_ref[0:block_width, :] = vt_ref[own, :]

    @pl.when((lax.axis_index('row') == 0) & (pl.program_id(0) == 0))
    def _():
        out_ref[0:block_width, 0:n] = rvt_ref[own, :]


def update(a_t, vt, yt, rvt, tau_line, tfac, block_width, tile=1024):
    local_cols, local_rows = a_t.shape
    n = vt.shape[0]
    once = lambda i: (0, 0)
    return pl.pallas_call(
        functools.partial(update_kernel, block_width),
        out_shape=(jax.ShapeDtypeStruct(a_t.shape, jnp.float32), jax.ShapeDtypeStruct(tau_line.shape, jnp.float32),
                   jax.ShapeDtypeStruct(tfac.shape, jnp.float32)),
        grid=(local_rows // tile,),
        in_specs=[pl.BlockSpec((local_cols, tile), lambda i: (0, i)), pl.BlockSpec((n, tile), lambda i: (0, i)),
                  pl.BlockSpec((local_cols, n), once), pl.BlockSpec((n, n), once), pl.BlockSpec((1, n), once),
                  pl.BlockSpec(tfac.shape, lambda i: (0, 0, 0))],
        out_specs=[pl.BlockSpec((local_cols, tile), lambda i: (0, i)), pl.BlockSpec((1, n), once),
                   pl.BlockSpec(tfac.shape, lambda i: (0, 0, 0))],
        scratch_shapes=[pltpu.VMEM((local_cols, 6 * n), jnp.bfloat16)],
        compiler_params=pltpu.CompilerParams(dimension_semantics=('arbitrary',), vmem_limit_bytes=56 * 1024 * 1024),
        name='update',
    )(a_t, vt, yt, rvt, tau_line, tfac)


def solution(mesh):
    col_count = mesh.shape['col']
    row_count = mesh.shape['row']
    assert col_count == PANELS == 4
    block_spec = P(('batch', 'row'), 'col', None)

    def device_fn(a_local):
        local_rows, local_blocks, block_width = a_local.shape
        width = PANELS * block_width
        local_cols = local_blocks * block_width
        a_t = a_local.transpose(1, 2, 0).reshape(local_cols, local_rows)
        kept, vt, yt, rvt, tau_line, tfac, redo = front(a_t, row_count, block_width)
        out_t, tau_line, tfac = update(a_t, vt, yt, rvt, tau_line, tfac, block_width)
        def column_form(state):
            kept = state[4]
            a_local = kept.reshape(local_blocks, block_width, local_rows).transpose(2, 0, 1)
            a_out, tau, tfac = columnwise_qr(a_local, col_count, row_count)
            return jnp.int32(0), a_out.transpose(1, 2, 0).reshape(local_cols, local_rows), tau, tfac, kept

        state = (redo[0, 0], out_t, tau_line[0], tfac, kept)
        _, out_t, tau, tfac, _ = lax.while_loop(lambda state: state[0] > 0, column_form, state)
        return out_t.reshape(local_blocks, block_width, local_rows).transpose(2, 0, 1), tau, tfac

    return jax.shard_map(device_fn, mesh=mesh, in_specs=(block_spec,), out_specs=(block_spec, P('batch'), P('batch', None, None)), check_vma=False)
```

```python
import functools
import math
import jax
import jax.numpy as jnp
from jax import lax
from jax.experimental import pallas as pl
from jax.experimental.pallas import tpu as pltpu
from jax.sharding import PartitionSpec as P

PANELS = 4
HIGHEST = lax.Precision.HIGHEST
MESH = pl.DeviceIdType.MESH
COND_MAX = 1.0e4
ABS_MAX = 1.0e15
GRAM_MIN = 1.0e-4


def mat_dot(left_mat, right_mat):
    return jnp.dot(left_mat, right_mat, precision=HIGHEST, preferred_element_type=jnp.float32)


def mat_einsum(einsum_form, left_mat, right_mat):
    return jnp.einsum(einsum_form, left_mat, right_mat, precision=HIGHEST, preferred_element_type=jnp.float32)


def axis_sum_kernel(axis, count, x_ref, out_ref, recv_buf, send_sem, recv_sem):
    me = lax.axis_index(axis)
    barrier = pltpu.get_barrier_semaphore()
    for step in range(1, count):
        pl.semaphore_signal(barrier, inc=1, device_id={axis: lax.rem(me + step, count)}, device_id_type=MESH)
    pl.semaphore_wait(barrier, count - 1)

    def copy(step, slot):
        return pltpu.make_async_remote_copy(
            src_ref=x_ref, dst_ref=recv_buf.at[slot], send_sem=send_sem.at[step], recv_sem=recv_sem.at[step],
            device_id={axis: lax.rem(me + step, count)}, device_id_type=MESH)

    for step in range(1, count):
        copy(step, me).start()
    recv_buf[me] = x_ref[...]
    for step in range(1, count):
        copy(step, lax.rem(me + count - step, count)).wait_recv()
    total = recv_buf[0]
    for i in range(1, count):
        total = total + recv_buf[i]
    out_ref[...] = total
    for step in range(1, count):
        copy(step, me).wait_send()


def axis_sum(x, axis, count, collective_id):
    size = math.prod(x.shape)
    lines = -(-size // 1024) * 8
    flat = jnp.pad(x.reshape(-1), (0, lines * 128 - size)).reshape(lines, 128)
    spec = pl.BlockSpec(memory_space=pltpu.VMEM)
    total = pl.pallas_call(
        functools.partial(axis_sum_kernel, axis, count),
        out_shape=jax.ShapeDtypeStruct(flat.shape, jnp.float32),
        in_specs=[spec],
        out_specs=spec,
        scratch_shapes=[pltpu.VMEM((count,) + flat.shape, jnp.float32), pltpu.SemaphoreType.DMA((count,)), pltpu.SemaphoreType.DMA((count,))],
        compiler_params=pltpu.CompilerParams(collective_id=collective_id, has_side_effects=True),
        name='axis_sum',
    )(flat)
    return total.reshape(-1)[:size].reshape(x.shape)


def apply_reflector(panel_work, tau_vec, column, col_idx, pivot_row, row_ids, tail_dots, pivot_line):
    col_ids = jnp.arange(panel_work.shape[1])
    alpha_val = lax.dynamic_index_in_dim(pivot_line, col_idx, keepdims=False)
    norm_val = jnp.sqrt(lax.dynamic_index_in_dim(tail_dots, col_idx, keepdims=False))
    beta_val = jnp.where(alpha_val >= 0.0, -norm_val, norm_val)
    tau_val = (beta_val - alpha_val) / beta_val
    scale_val = 1.0 / (alpha_val - beta_val)
    refl_vec = jnp.where(row_ids > pivot_row, column * scale_val, jnp.where(row_ids == pivot_row, 1.0, 0.0))
    refl_dot = scale_val * (tail_dots - alpha_val * pivot_line) + pivot_line
    refl_dot = jnp.where(col_ids > col_idx, refl_dot, 0.0)
    new_col = jnp.where(row_ids < pivot_row, column, jnp.where(row_ids == pivot_row, beta_val, refl_vec))
    panel_work = jnp.where(col_ids[None, :] == col_idx, new_col[:, None], panel_work - tau_val * refl_vec[:, None] * refl_dot[None, :])
    tau_vec = jnp.where(col_ids == col_idx, tau_val, tau_vec)
    return panel_work, tau_vec


def factor_panel_rows(panel_in, row_base, pivot_base, row_count):
    local_rows, block_width = panel_in.shape
    row_ids = row_base + jnp.arange(local_rows)

    def column_step(col_idx, loop_state):
        panel_work, tau_vec = loop_state
        pivot_row = pivot_base + col_idx
        column = lax.dynamic_index_in_dim(panel_work, col_idx, axis=1, keepdims=False)
        tail_col = jnp.where(row_ids >= pivot_row, column, 0.0)
        local_pivot = jnp.clip(pivot_row - row_base, 0, local_rows - 1)
        holds_pivot = (pivot_row >= row_base) & (pivot_row < row_base + local_rows)
        pivot_line = lax.dynamic_index_in_dim(panel_work, local_pivot, axis=0, keepdims=False)
        pivot_line = jnp.where(holds_pivot, pivot_line, 0.0)
        packed = jnp.concatenate([mat_dot(tail_col[None, :], panel_work)[0], pivot_line])
        packed = axis_sum(packed, 'row', row_count, 1)
        return apply_reflector(panel_work, tau_vec, column, col_idx, pivot_row, row_ids, packed[:block_width], packed[block_width:])

    return lax.fori_loop(0, block_width, column_step, (panel_in, jnp.zeros((block_width,), jnp.float32)))


def tfactor_from_gram(gram_mat, tau_vec):
    block_width = gram_mat.shape[0]
    col_ids = jnp.arange(block_width)
    step_mat = -tau_vec[:, None] * jnp.where(col_ids[None, :] > col_ids[:, None], gram_mat, 0.0)
    eye_mat = jnp.eye(block_width, dtype=jnp.float32)
    inv_acc = eye_mat + step_mat
    power_mat = step_mat
    for _ in range(max(1, math.ceil(math.log2(block_width))) - 1):
        power_mat = mat_dot(power_mat, power_mat)
        inv_acc = mat_dot(inv_acc, eye_mat + power_mat)
    return inv_acc * tau_vec[None, :]


def columnwise_qr(a_local, col_count, row_count):
    local_rows, local_blocks, block_width = a_local.shape
    col_rank = lax.axis_index('col')
    row_base = lax.axis_index('row') * local_rows
    row_ids = row_base + jnp.arange(local_rows)
    col_ids = jnp.arange(block_width)
    global_ids = jnp.arange(local_blocks) * col_count + col_rank

    def panel_step(panel_idx, loop_state):
        a_local, tau_out, tfac_out = loop_state
        owner_col = panel_idx % col_count
        pivot_ids = panel_idx * block_width + col_ids
        panel_in = lax.dynamic_index_in_dim(a_local, panel_idx // col_count, axis=1, keepdims=False)
        panel_out, tau_vec = factor_panel_rows(panel_in, row_base, panel_idx * block_width, row_count)
        refl_mat = jnp.where(row_ids[:, None] > pivot_ids[None, :], panel_out, jnp.where(row_ids[:, None] == pivot_ids[None, :], 1.0, 0.0))
        gram_mat = axis_sum(mat_einsum('rk,rj->kj', refl_mat, refl_mat), 'row', row_count, 2)
        t_factor = tfactor_from_gram(gram_mat, tau_vec)
        packed = jnp.concatenate([refl_mat, t_factor], axis=0)
        packed = axis_sum(jnp.where(col_rank == owner_col, packed, 0.0), 'col', col_count, 3)
        refl_mat = packed[:local_rows]
        t_factor = packed[local_rows:]
        w_summed = axis_sum(mat_einsum('rk,rbc->kbc', refl_mat, a_local), 'row', row_count, 4)
        w_mat = mat_einsum('kj,kbc->jbc', t_factor, w_summed)
        w_mat = jnp.where((global_ids > panel_idx)[None, :, None], w_mat, 0.0)
        a_local = a_local - mat_einsum('rj,jbc->rbc', refl_mat, w_mat)
        a_local = jnp.where((global_ids == panel_idx)[None, :, None], panel_out[:, None, :], a_local)
        tau_out = lax.dynamic_update_index_in_dim(tau_out, jnp.diagonal(t_factor), panel_idx, 0)
        tfac_out = lax.dynamic_update_index_in_dim(tfac_out, t_factor, panel_idx, 0)
        return a_local, tau_out, tfac_out

    zero_tau = jnp.zeros((PANELS, block_width), jnp.float32)
    zero_tfac = jnp.zeros((PANELS, block_width, block_width), jnp.float32)
    a_local, tau_out, tfac_out = lax.fori_loop(0, PANELS, panel_step, (a_local, zero_tau, zero_tfac))
    return a_local, tau_out.reshape(-1), tfac_out


CHUNKS = 4
CROSS_ROWS = 512
SUB = 4
ROWS = 512


def dot_nn(left_mat, right_mat):
    return lax.dot_general(left_mat, right_mat, (((1,), (0,)), ((), ())), precision=HIGHEST, preferred_element_type=jnp.float32)


def split3(mat):
    hi = mat.astype(jnp.bfloat16)
    rest = mat - hi.astype(jnp.float32)
    mid = rest.astype(jnp.bfloat16)
    return hi, mid, (rest - mid.astype(jnp.float32)).astype(jnp.bfloat16)


def bf_nn(left_mat, right_mat):
    return lax.dot_general(left_mat, right_mat, (((1,), (0,)), ((), ())), preferred_element_type=jnp.float32)


def bf_nt(left_mat, right_mat):
    return lax.dot_general(left_mat, right_mat, (((1,), (1,)), ((), ())), preferred_element_type=jnp.float32)


def dot_nt(left_mat, right_mat):
    return lax.dot_general(left_mat, right_mat, (((1,), (1,)), ((), ())), precision=HIGHEST, preferred_element_type=jnp.float32)


def factor_steps(w1_ref, w2_ref, vinv_ref, v_ref, r_ref, u_ref):
    n = vinv_ref.shape[0]
    row_col = lax.broadcasted_iota(jnp.int32, (n, 1), 0)
    lane_ids = lax.broadcasted_iota(jnp.int32, (n, n), 1)
    lane8 = lax.broadcasted_iota(jnp.int32, (8, n), 1)
    sub_col = lax.broadcasted_iota(jnp.int32, (8, 1), 0)
    line_ids = lax.broadcasted_iota(jnp.int32, (1, n), 1)

    def pick(mask, mat):
        return jnp.sum(jnp.where(mask, mat, 0.0), axis=1, keepdims=True)

    def step(b, tau_line):
        base = pl.multiple_of(b * 8, 8)
        rows8 = pl.ds(base, 8)
        for first in range(0, 8, SUB):
            tile1, tile2 = w1_ref[rows8, :], w2_ref[rows8, :]
            ks = [base + first + j for j in range(SUB)]
            d1 = [pick(lane8 == k, tile1) for k in ks]
            d2 = [pick(lane8 == k, tile2) for k in ks]
            w1, w2 = w1_ref[...], w2_ref[...]
            c1 = [pick(lane_ids == k, w1) for k in ks]
            c2 = [pick(lane_ids == k, w2) for k in ks]
            below = row_col >= base + 8
            v_mat = v_ref[...]
            for j in range(SUB):
                at, k = first + j, ks[j]
                alpha, norm_sq = d1[j][at:at + 1], d2[j][at:at + 1]
                norm = jnp.sqrt(norm_sq)
                beta = jnp.where(alpha >= 0.0, -norm, norm)
                beta_rec = 1.0 / beta
                pivot_rec = 1.0 / (alpha - beta)
                line1, line2 = tile1[at:at + 1, :], tile2[at:at + 1, :]
                here, after = line_ids == k, line_ids > k
                tau_line = jnp.where(here, (beta - alpha) * beta_rec, tau_line)
                r_tail = jnp.where(after, line2 * beta_rec, 0.0)
                u_tail = jnp.where(after, line1 - r_tail, 0.0)
                low = jnp.where(line_ids < k, line1, 0.0)
                r_ref[pl.ds(k, 1), :] = jnp.where(here, beta, r_tail)
                u_ref[pl.ds(k, 1), :] = jnp.where(here, alpha - beta, u_tail)
                vinv_ref[pl.ds(k, 1), :] = jnp.where(here, 1.0, low)
                m1 = jnp.where(sub_col == at, pivot_rec, d1[j] * pivot_rec)
                m2 = jnp.where(sub_col == at, beta_rec, d2[j] * beta_rec)
                f1, f2 = c1[j] * pivot_rec, c2[j] * beta_rec
                for t in range(j + 1, SUB):
                    r_val = d2[t][at:at + 1] * beta_rec
                    u_val = d1[t][at:at + 1] - r_val
                    d1[t] = jnp.where(sub_col == at, 0.0, d1[t]) - m1 * u_val
                    d2[t] = jnp.where(sub_col == at, 0.0, d2[t]) - m2 * r_val
                    c1[t] = c1[t] - f1 * u_val
                    c2[t] = c2[t] - f2 * r_val
                here8 = lane8 == k
                rest8 = sub_col > at
                tile1 = jnp.where(here8, jnp.where(rest8, -m1, m1),
                                  jnp.where(sub_col == at, 0.0, tile1) - m1 * jnp.where(rest8, u_tail + low, u_tail))
                tile2 = jnp.where(here8, m2, jnp.where(sub_col == at, 0.0, tile2) - m2 * r_tail)
                v8 = jnp.where(rest8, m1, 0.0)
                at_col = lane_ids == k
                w1 = jnp.where(at_col, jnp.where(below, -f1, f1), w1 - f1 * jnp.where(below, u_tail + low, u_tail))
                w2 = jnp.where(at_col, f2, w2 - f2 * r_tail)
                v_mat = jnp.where(at_col, f1, v_mat)
                v_rows = jnp.where(here8, v8, v_ref[rows8, :] if j == 0 else v_rows)
            w1_ref[...] = w1
            w2_ref[...] = w2
            v_ref[...] = v_mat
            w1_ref[rows8, :] = tile1
            w2_ref[rows8, :] = tile2
            v_ref[rows8, :] = v_rows
        return tau_line

    return lax.fori_loop(0, n // 8, step, jnp.zeros((1, n), jnp.float32))


def front_kernel(row_count, block_width, a_hbm, a_copy, a_buf, vt_hbm, yt_out, rvt_out, tau_out, tf_out, flag_out,
                 lead, ct_acc, g_acc, g_send, g_recv, g_part, g_all, c_recv, top_t, a11_t, yt_buf, max_buf,
                 w1_ref, w2_ref, vinv_ref, v_ref, r_ref, u_ref,
                 vt_out, vt_sem, own_sem, load_sem, keep_sem, right_send, left_send, fwd_send, from_left, from_right, fwd_recv,
                 max_send, max_recv, a11_send, a11_recv, top_send, top_recv,
                 gs_send, gs_recv, ga_send, ga_recv, cs_send, cs_recv, y_send, y_recv):
    local_cols, local_rows = a_hbm.shape
    n = PANELS * block_width
    chunk = local_rows // CHUNKS
    share = local_cols // row_count
    g_rows = n // row_count
    row_rank = lax.axis_index('row')
    col_rank = lax.axis_index('col')
    right_col, left_col, far_col = lax.rem(col_rank + 1, 4), lax.rem(col_rank + 3, 4), lax.rem(col_rank + 2, 4)

    def lanes(c):
        return pl.ds(pl.multiple_of(c * chunk, chunk), chunk)

    def panel(p):
        return pl.ds(pl.multiple_of(p * block_width, block_width), block_width)

    def peer_of(step):
        return lax.rem(row_rank + step, row_count)

    def own_copy(c):
        return pltpu.make_async_copy(a_hbm.at[0:block_width, lanes(c)], lead.at[panel(col_rank), lanes(c)], own_sem.at[c])

    def load_copy(c):
        return pltpu.make_async_copy(a_hbm.at[:, lanes(c)], a_buf.at[:, lanes(c)], load_sem.at[c])

    def keep_copy(c):
        return pltpu.make_async_copy(a_buf.at[:, lanes(c)], a_copy.at[:, lanes(c)], keep_sem.at[c])

    def to_col(c, owner, target, send_sem, recv_sem):
        return pltpu.make_async_remote_copy(
            src_ref=lead.at[panel(owner), lanes(c)], dst_ref=lead.at[panel(owner), lanes(c)],
            send_sem=send_sem.at[c], recv_sem=recv_sem.at[c], device_id={'col': target}, device_id_type=MESH)

    def to_row(src_ref, dst_ref, send_sem, recv_sem, target):
        return pltpu.make_async_remote_copy(
            src_ref=src_ref, dst_ref=dst_ref, send_sem=send_sem, recv_sem=recv_sem,
            device_id={'row': target}, device_id_type=MESH)

    def send_right(c):
        return to_col(c, col_rank, right_col, right_send, from_left)

    def send_left(c):
        return to_col(c, col_rank, left_col, left_send, from_right)

    @pl.loop(0, CHUNKS)
    def _(c):
        own_copy(c).start()

    @pl.loop(0, CHUNKS)
    def _(c):
        load_copy(c).start()

    barrier = pltpu.get_barrier_semaphore()
    for step in range(1, row_count):
        pl.semaphore_signal(barrier, inc=1, device_id={'row': peer_of(step)}, device_id_type=MESH)
    for step in range(1, 4):
        pl.semaphore_signal(barrier, inc=1, device_id={'col': lax.rem(col_rank + step, 4)}, device_id_type=MESH)
    pl.semaphore_wait(barrier, row_count - 1 + 3)

    def top_copy(target):
        return to_row(a_hbm.at[pl.ds(pl.multiple_of(target * share, share), share), 0:n], top_t, top_send.at[target], top_recv, target)

    def a11_copy(target):
        return to_row(lead.at[:, 0:n], a11_t, a11_send.at[target], a11_recv, target)

    for c in range(2):
        own_copy(c).wait()
        send_right(c).start()
        send_left(c).start()
    g_acc[...] = jnp.zeros_like(g_acc)
    ct_acc[...] = jnp.zeros_like(ct_acc)

    def cross_step(c):
        hi, mid, lo = split3(lead[:, lanes(c)])
        hi_mid = jnp.concatenate([hi, mid], axis=0)
        hi_mid = jnp.concatenate([hi_mid, hi_mid], axis=1)
        hi_lo = jnp.concatenate([hi, lo], axis=1)

        @pl.loop(0, local_cols // CROSS_ROWS)
        def _(i):
            at_rows = pl.ds(pl.multiple_of(i * CROSS_ROWS, CROSS_ROWS), CROSS_ROWS)
            a_hi, a_mid, a_lo = split3(a_buf[at_rows, lanes(c)])
            pair = bf_nt(jnp.concatenate([a_mid, a_hi], axis=1), hi_mid)
            rest = bf_nt(jnp.concatenate([a_lo, a_hi], axis=1), hi_lo)
            ct_acc[at_rows, :] = ct_acc[at_rows, :] + (pair[:, 0:n] + (pair[:, n:] + rest))

    def abs_max(c):
        part = jnp.abs(a_buf[:, lanes(c)])
        return jnp.max(jnp.max(part.reshape(local_cols // 8, 8, chunk), axis=0).reshape(8, chunk // 128, 128), axis=1)

    def max_copy(step):
        target = lax.rem(col_rank + step, 4)
        return pltpu.make_async_remote_copy(
            src_ref=max_buf.at[0], dst_ref=max_buf.at[step], send_sem=max_send.at[step], recv_sem=max_recv.at[step],
            device_id={'col': target}, device_id_type=MESH)

    max_buf[0] = jnp.zeros((8, 128), jnp.float32)

    @pl.loop(0, CHUNKS + 1)
    def _(c):
        @pl.when(c + 2 < CHUNKS)
        def _():
            own_copy(c + 2).wait()
            send_right(c + 2).start()
            send_left(c + 2).start()

        @pl.when(c < CHUNKS)
        def _():
            to_col(c, left_col, right_col, right_send, from_left).wait_recv()
            to_col(c, right_col, left_col, left_send, from_right).wait_recv()

            @pl.when(lax.rem(c, 2) == 0)
            def _():
                to_col(c, left_col, right_col, fwd_send, fwd_recv).start()

            @pl.when(lax.rem(c, 2) == 1)
            def _():
                to_col(c, right_col, left_col, fwd_send, fwd_recv).start()
            load_copy(c).wait()
            keep_copy(c).start()
            max_buf[0] = jnp.maximum(max_buf[0], abs_max(c))

        @pl.when(c > 0)
        def _():
            to_col(c - 1, far_col, right_col, fwd_send, fwd_recv).wait_recv()
            part = lead[:, lanes(c - 1)]
            g_acc[...] = g_acc[...] + dot_nt(part, part)

        @pl.when(c == 1)
        def _():
            @pl.when(row_rank == 0)
            def _():
                for target in range(1, row_count):
                    top_copy(target).start()
                    a11_copy(target).start()

        @pl.when(c == CHUNKS - 1)
        def _():
            for step in range(1, 4):
                max_copy(step).start()

        @pl.when((c > 0) & (c < CHUNKS))
        def _():
            cross_step(c - 1)

    for step in range(1, 4):
        max_copy(step).wait_recv()
    big = jnp.maximum(jnp.maximum(max_buf[0], max_buf[1]), jnp.maximum(max_buf[2], max_buf[3]))
    for i in range(row_count):
        g_send[i, 0:g_rows] = g_acc[i * g_rows:(i + 1) * g_rows, :]
        g_send[i, g_rows:g_rows + 8] = big

    def gs_copy(step):
        return to_row(g_send.at[peer_of(step)], g_recv.at[row_rank], gs_send.at[step], gs_recv.at[step], peer_of(step))

    def ga_copy(step):
        return to_row(g_part, g_all.at[row_rank], ga_send.at[step], ga_recv.at[step], peer_of(step))

    def cs_copy(step):
        at_rows = pl.ds(pl.multiple_of(peer_of(step) * share, share), share)
        return to_row(ct_acc.at[at_rows, :], c_recv.at[row_rank], cs_send.at[step], cs_recv.at[step], peer_of(step))

    my_share = pl.ds(pl.multiple_of(row_rank * share, share), share)

    partner = row_rank + 1 - 2 * lax.rem(row_rank, 2)

    def y_rows(owner):
        return pl.ds(pl.multiple_of(owner * share, share), share)

    def y_copy(step):
        target = partner if step == 0 else peer_of(step)
        return to_row(yt_buf.at[my_share, :], yt_buf.at[my_share, :], y_send.at[step], y_recv.at[step], target)

    def y_pass(step):
        source = lax.rem(row_rank + row_count - step, row_count)
        return to_row(yt_buf.at[y_rows(source), :], yt_buf.at[y_rows(source), :], y_send.at[step + 1], y_recv.at[step + 1], partner)

    def y_arrive(owner, slot):
        to_row(yt_buf.at[y_rows(owner), :], yt_buf.at[y_rows(owner), :], y_send.at[slot], y_recv.at[slot], partner).wait_recv()

    def arrived(send_kind, buf, sems, step):
        source = lax.rem(row_rank + row_count - step, row_count)
        to_row(buf.at[source], buf.at[source], send_kind.at[step], sems.at[step], source).wait_recv()

    for step in range(1, row_count):
        gs_copy(step).start()
    g_recv[row_rank] = g_send[row_rank]

    cross_step(CHUNKS - 1)
    for step in range(1, row_count):
        arrived(gs_send, g_recv, gs_recv, step)
    total = g_recv[0, 0:g_rows]
    big = g_recv[0, g_rows:g_rows + 8]
    for i in range(1, row_count):
        total = total + g_recv[i, 0:g_rows]
        big = jnp.maximum(big, g_recv[i, g_rows:g_rows + 8])
    g_part[0:g_rows] = total
    g_part[g_rows:g_rows + 8] = big
    for step in range(1, row_count):
        ga_copy(step).start()
    g_all[row_rank] = g_part[...]

    for step in range(1, row_count):
        cs_copy(step).start()
    c_recv[row_rank] = ct_acc[my_share, :]
    for step in range(1, row_count):
        arrived(ga_send, g_all, ga_recv, step)

    @pl.when(row_rank == 0)
    def _():
        a11_t[...] = lead[:, 0:n]
        top_t[...] = a_buf[0:share, 0:n]

    @pl.when(row_rank > 0)
    def _():
        a11_copy(row_rank).wait_recv()
        top_copy(row_rank).wait_recv()

    row_ids = lax.broadcasted_iota(jnp.int32, (n, n), 0)
    lane_ids = lax.broadcasted_iota(jnp.int32, (n, n), 1)
    eye = jnp.where(row_ids == lane_ids, 1.0, 0.0)
    big = g_all[0, g_rows:g_rows + 8]
    for i in range(row_count):
        g_acc[i * g_rows:(i + 1) * g_rows, :] = g_all[i, 0:g_rows]
        big = jnp.maximum(big, g_all[i, g_rows:g_rows + 8])
    w1_ref[...] = a11_t[...].T
    w2_ref[...] = g_acc[...]
    v_ref[...] = jnp.zeros((n, n), jnp.float32)
    tau_out[...] = factor_steps(w1_ref, w2_ref, vinv_ref, v_ref, r_ref, u_ref)
    u_inv = w1_ref[...]
    r_inv = w2_ref[...]

    for step in range(1, row_count):
        arrived(cs_send, c_recv, cs_recv, step)
    cross = c_recv[0]
    for i in range(1, row_count):
        cross = cross + c_recv[i]
    yt_buf[my_share, :] = dot_nt(top_t[...] - dot_nn(cross, r_inv), vinv_ref[...])
    for step in range(0, row_count, 2):
        y_copy(step).start()

    diag = jnp.sum(jnp.where(row_ids == lane_ids, g_acc[...], 0.0), axis=1, keepdims=True)
    cond_val = jnp.sum(jnp.sum(diag * r_inv * r_inv, axis=1, keepdims=True), axis=0, keepdims=True)
    big_val = jnp.max(jnp.max(big, axis=1, keepdims=True), axis=0, keepdims=True)
    low_val = jnp.min(diag, axis=0, keepdims=True)
    usable = (cond_val < COND_MAX) & (big_val < ABS_MAX) & (low_val > GRAM_MIN)
    flag_out[0, 0] = jnp.max(jnp.where(usable, 0, 1))
    t_full = -dot_nn(u_ref[...], dot_nt(r_inv, vinv_ref[...]))
    for p in range(PANELS):
        tf_out[p] = t_full[p * block_width:(p + 1) * block_width, p * block_width:(p + 1) * block_width]
    rv_t = jnp.where(lane_ids < row_ids, v_ref[...], r_ref[...]).T
    rvt_out[...] = rv_t
    u_inv_t = u_inv.T

    @pl.loop(0, CHUNKS)
    def _(c):
        vt_out[:, lanes(c)] = dot_nn(u_inv_t, lead[:, lanes(c)])

    @pl.when(row_rank == 0)
    def _():
        vt_out[:, 0:n] = jnp.where(lane_ids > row_ids, rv_t, eye)

    vt_copy = pltpu.make_async_copy(vt_out, vt_hbm, vt_sem)
    vt_copy.start()
    for step in range(2, row_count, 2):
        y_arrive(lax.rem(row_rank + row_count - step, row_count), step)
        y_pass(step).start()
    y_arrive(partner, 0)
    for step in range(2, row_count, 2):
        y_arrive(lax.rem(partner + row_count - step, row_count), step + 1)
    yt_out[...] = yt_buf[...]
    vt_copy.wait()

    @pl.loop(0, CHUNKS)
    def _(c):
        send_right(c).wait_send()
        send_left(c).wait_send()
        to_col(c, left_col, right_col, fwd_send, fwd_recv).wait_send()
        keep_copy(c).wait()
    for step in range(1, 4):
        max_copy(step).wait_send()
    for step in range(1, row_count):
        gs_copy(step).wait_send()
        ga_copy(step).wait_send()
        cs_copy(step).wait_send()
    y_copy(0).wait_send()
    for step in range(2, row_count, 2):
        y_copy(step).wait_send()
        y_pass(step).wait_send()

    @pl.when(row_rank == 0)
    def _():
        for target in range(1, row_count):
            top_copy(target).wait_send()
            a11_copy(target).wait_send()


def front(a_t, row_count, block_width):
    local_cols, local_rows = a_t.shape
    n = PANELS * block_width
    share = local_cols // row_count
    g_rows = n // row_count
    f32 = jnp.float32
    mat = jax.ShapeDtypeStruct((n, n), f32)
    vmem, sem = pltpu.VMEM, pltpu.SemaphoreType.DMA
    spec = pl.BlockSpec(memory_space=pltpu.VMEM)
    return pl.pallas_call(
        functools.partial(front_kernel, row_count, block_width),
        out_shape=(jax.ShapeDtypeStruct(a_t.shape, f32), jax.ShapeDtypeStruct(a_t.shape, f32), jax.ShapeDtypeStruct((n, local_rows), f32), jax.ShapeDtypeStruct((local_cols, n), f32), mat,
                   jax.ShapeDtypeStruct((1, n), f32), jax.ShapeDtypeStruct((PANELS, block_width, block_width), f32),
                   jax.ShapeDtypeStruct((1, 1), jnp.int32)),
        in_specs=[pl.BlockSpec(memory_space=pl.ANY)],
        out_specs=[pl.BlockSpec(memory_space=pl.ANY), spec, pl.BlockSpec(memory_space=pl.ANY)] + [spec] * 4 + [pl.BlockSpec(memory_space=pltpu.SMEM)],
        scratch_shapes=[
            vmem((n, local_rows), f32), vmem((local_cols, n), f32), vmem((n, n), f32),
            vmem((row_count, g_rows + 8, n), f32), vmem((row_count, g_rows + 8, n), f32), vmem((g_rows + 8, n), f32),
            vmem((row_count, g_rows + 8, n), f32), vmem((row_count, share, n), f32), vmem((share, n), f32), vmem((n, n), f32),
            vmem((local_cols, n), f32), vmem((4, 8, 128), f32),
            vmem((n, n), f32), vmem((n, n), f32), vmem((n, n), f32), vmem((n, n), f32), vmem((n, n), f32), vmem((n, n), f32),
            vmem((n, local_rows), f32), sem,
            sem((CHUNKS,)), sem((CHUNKS,)), sem((CHUNKS,)), sem((CHUNKS,)), sem((CHUNKS,)), sem((CHUNKS,)), sem((CHUNKS,)), sem((CHUNKS,)), sem((CHUNKS,)),
            sem((4,)), sem((4,)), sem((row_count,)), sem, sem((row_count,)), sem,
            sem((row_count,)), sem((row_count,)), sem((row_count,)), sem((row_count,)),
            sem((row_count,)), sem((row_count,)), sem((row_count,)), sem((row_count,)),
        ],
        compiler_params=pltpu.CompilerParams(collective_id=0, has_side_effects=True, vmem_limit_bytes=26 * 1024 * 1024),
        name='front',
    )(a_t)


def update_kernel(block_width, a_ref, vt_ref, yt_ref, rvt_ref, tau_ref, tf_ref, out_ref, tau_out, tf_out, y_parts):
    n, tile = vt_ref.shape
    local_cols = a_ref.shape[0]
    own = pl.ds(pl.multiple_of(lax.axis_index('col') * block_width, block_width), block_width)

    @pl.when(pl.program_id(0) == 0)
    def _():
        tau_out[...] = tau_ref[...]
        tf_out[...] = tf_ref[...]
        for first in range(0, local_cols, ROWS):
            hi, mid, lo = split3(yt_ref[first:first + ROWS, :])
            y_parts[first:first + ROWS, :] = jnp.concatenate([hi, lo, mid, mid, hi, hi], axis=1)

    for lane in range(0, tile, ROWS):
        a_lanes = pl.ds(pl.multiple_of(pl.program_id(0) * tile + lane, ROWS), ROWS)
        hi, mid, lo = split3(vt_ref[:, lane:lane + ROWS])
        vt_parts = jnp.concatenate([lo, hi, mid, hi, mid, hi], axis=0)
        for first in range(0, local_cols, ROWS):
            prod = bf_nn(y_parts[first:first + ROWS, :], vt_parts)
            out_ref[first:first + ROWS, lane:lane + ROWS] = a_ref[first:first + ROWS, a_lanes] - prod
    out_ref[0:block_width, :] = vt_ref[own, :]

    @pl.when((lax.axis_index('row') == 0) & (pl.program_id(0) == 0))
    def _():
        out_ref[0:block_width, 0:n] = rvt_ref[own, :]


def update(a_t, vt, yt, rvt, tau_line, tfac, block_width, tile=1024):
    local_cols, local_rows = a_t.shape
    n = vt.shape[0]
    once = lambda i: (0, 0)
    return pl.pallas_call(
        functools.partial(update_kernel, block_width),
        out_shape=(jax.ShapeDtypeStruct(a_t.shape, jnp.float32), jax.ShapeDtypeStruct(tau_line.shape, jnp.float32),
                   jax.ShapeDtypeStruct(tfac.shape, jnp.float32)),
        grid=(local_rows // tile,),
        in_specs=[pl.BlockSpec(memory_space=pltpu.VMEM), pl.BlockSpec((n, tile), lambda i: (0, i)),
                  pl.BlockSpec((local_cols, n), once), pl.BlockSpec((n, n), once), pl.BlockSpec((1, n), once),
                  pl.BlockSpec(tfac.shape, lambda i: (0, 0, 0))],
        out_specs=[pl.BlockSpec((local_cols, tile), lambda i: (0, i)), pl.BlockSpec((1, n), once),
                   pl.BlockSpec(tfac.shape, lambda i: (0, 0, 0))],
        scratch_shapes=[pltpu.VMEM((local_cols, 6 * n), jnp.bfloat16)],
        compiler_params=pltpu.CompilerParams(dimension_semantics=('arbitrary',), vmem_limit_bytes=26 * 1024 * 1024),
        name='update',
    )(a_t, vt, yt, rvt, tau_line, tfac)


def solution(mesh):
    col_count = mesh.shape['col']
    row_count = mesh.shape['row']
    assert col_count == PANELS == 4
    block_spec = P(('batch', 'row'), 'col', None)

    def device_fn(a_local):
        local_rows, local_blocks, block_width = a_local.shape
        width = PANELS * block_width
        local_cols = local_blocks * block_width
        a_t = a_local.transpose(1, 2, 0).reshape(local_cols, local_rows)
        kept, a_near, vt, yt, rvt, tau_line, tfac, redo = front(a_t, row_count, block_width)
        out_t, tau_line, tfac = update(a_near, vt, yt, rvt, tau_line, tfac, block_width)
        def column_form(state):
            kept = state[4]
            a_local = kept.reshape(local_blocks, block_width, local_rows).transpose(2, 0, 1)
            a_out, tau, tfac = columnwise_qr(a_local, col_count, row_count)
            return jnp.int32(0), a_out.transpose(1, 2, 0).reshape(local_cols, local_rows), tau, tfac, kept

        state = (redo[0, 0], out_t, tau_line[0], tfac, kept)
        _, out_t, tau, tfac, _ = lax.while_loop(lambda state: state[0] > 0, column_form, state)
        return out_t.reshape(local_blocks, block_width, local_rows).transpose(2, 0, 1), tau, tfac

    return jax.shard_map(device_fn, mesh=mesh, in_specs=(block_spec,), out_specs=(block_spec, P('batch'), P('batch', None, None)), check_vma=False)
```
